512 devices in a mesh: pipe: 16 (over x_lo, y), dp: 4 (over x_hi, core), expert: 8 (over z).
Axes of the slice: x: 4 (x_hi: 2, x_lo: 2; x = x_hi * 2 + x_lo), y: 8, z: 8, core: 2. Of those that a mesh axis runs over, the one named last changes fastest.
Arguments:
- entering: bfloat16 [16, 512, 4096], P('pipe', 'dp', 'expert'), may hold values from -6 to 6
- pending: bfloat16 [16, 512, 4096], P('pipe', 'dp', 'expert'), may hold values from -6 to 6
- stashed_in: bfloat16 [16, 512, 4096], P('pipe', 'dp', 'expert'), may hold values from -6 to 6
- forward_routes: int32 [16, 512, 2], P('pipe', 'dp'), may hold values from 0 to 3, all different within a row; in each aligned block of 128 rows (0 to 127, 128 to 255, ..., all dimensions but the last counted through in order) at most 64 rows name the same one
- backward_routes: int32 [16, 512, 2], P('pipe', 'dp'), may hold values from 0 to 3, all different within a row; in each aligned block of 128 rows (0 to 127, 128 to 255, ..., all dimensions but the last counted through in order) at most 64 rows name the same one
- norm_gains: float32 [16, 4096], P('pipe', 'expert'), may hold values from 0.5 to 1.5
- w_router: bfloat16 [16, 4096, 4], P('pipe', 'expert'), may hold values from -0.09375 to 0.09375
- w_gateup: bfloat16 [16, 4, 4096, 2, 1024], P('pipe', 'dp', None, None, 'expert'), may hold values from -0.09375 to 0.09375
- w_down: bfloat16 [16, 4, 1024, 4096], P('pipe', 'dp', 'expert'), may hold values from -0.1875 to 0.1875
Outputs:
- forward_out: bfloat16 [16, 512, 4096], P('pipe', 'dp', 'expert')
- input_grads: bfloat16 [16, 512, 4096], P('pipe', 'dp', 'expert')
- passed_forward: bfloat16 [16, 512, 4096], P('pipe', 'dp', 'expert')
- passed_backward: bfloat16 [16, 512, 4096], P('pipe', 'dp', 'expert')
- gain_grads: float32 [16, 4096], P('pipe', 'expert')
The draws below stay inside these ranges and needn't reach their ends.
Inputs may be any that keep to these rules, and one draw needn't show every extreme that they name: `forward_routes`: each row names 2 different experts; in each aligned block of 128 rows (one sequence) every expert is named by exactly 64 rows. `backward_routes`: each row names 2 different experts; in each aligned block of 128 rows (one sequence) every expert is named by exactly 64 rows.
All inputs are finite; a program needn't handle non-finite values.
Results may differ from the reference program's by a relative error of at most 0.015.
Values may be sent and summed in bfloat16 or wider, within the bound.
No kernel may reach another device: no remote copies, remote signals or barrier semaphores. Data moves between devices by JAX's collectives and lax.ppermute only.
A program may use at most 64 MiB of HBM per device.

```python
import math
import jax
import jax.numpy as jnp
import numpy as np
from jax import lax

D = 4096
FF = 1024
TOPK = 2
TOK = 128
EXPERTS = 4
TOKENS = 512
CAP = 64
N_PIPE = 16
N_EXPERT = 8


def shard_levels(stream_key, dims, split, least, high):
    factor_of, own = 1.0, jax.random.fold_in(stream_key, 6)
    for dim, shards_of in split:
        heights = jnp.exp(jax.random.uniform(jax.random.fold_in(own, dim), (shards_of,), jnp.float32, least / len(split), high / len(split)))
        factor_of = factor_of * jnp.repeat(heights, dims[dim] // shards_of).reshape([-1 if axis == dim else 1 for axis in range(len(dims))])
    return factor_of


def shared_out(stream_key, own, number, rows, count, top, most, skew):
    order = jax.random.permutation(stream_key, count)
    packed, ordinary = portions_of(count, rows * top, most, skew, True), portions_of(count, rows * top, most, skew, False)
    places = jnp.arange(count)

    def named(lengths, offset_by):
        used = int((lengths > 0).sum())
        fixed = max(1, used // 4)
        shifted = fixed + (places - fixed + offset_by * (used - fixed)) % max(1, count - fixed)
        return jnp.zeros((count,), jnp.int32).at[order[jnp.where(places < fixed, places, shifted)]].set(jnp.asarray(lengths, jnp.int32))

    lengths = jnp.where(number % 4 == 0, named(packed, number // 4), named(ordinary, number - number // 4 - 1))
    mixed = jax.random.permutation(jax.random.fold_in(own, 3), count)
    source_of, receiver = mixed[0:count // 2 * 2:2], mixed[1:count // 2 * 2:2]
    room = jnp.minimum(lengths[source_of] - 1, most - lengths[receiver]) // 2
    room = jnp.where((source_of == order[0]) | (receiver == order[0]) | (lengths[receiver] == 0), 0, jnp.maximum(room, 0))
    shifted = jax.random.randint(jax.random.fold_in(own, 4), (count // 2,), 0, 1 << 20) % (room + 1)
    lengths = lengths.at[source_of].add(-shifted).at[receiver].add(shifted)
    items = jnp.searchsorted(jnp.cumsum(lengths), jnp.arange(rows * top), side="right").astype(jnp.int32)
    listing = items.reshape(top, rows).T
    listing = listing[jax.random.permutation(jax.random.fold_in(own, 1), rows)]
    offset_by = jax.random.randint(jax.random.fold_in(own, 2), (rows, 1), 0, top)
    return jnp.take_along_axis(listing, (jnp.arange(top)[None, :] + offset_by) % top, axis=1)


def portions_of(amount, total, limit, slope, full):
    portions = [(1 << 20) // math.isqrt(grade ** slope) + 1 for grade in range(1, amount + 1)]
    largest = limit if full else min(limit, max(-(-total // amount), total * portions[0] // sum(portions)))
    least = 1 if total - largest >= amount - 1 else 0
    holding, spare = [largest] + [least] * (amount - 1), total - largest - least * (amount - 1)
    while spare > 0:
        movable = [i for i in range(1, amount) if holding[i] < largest] or [i for i in range(1, amount) if holding[i] < limit]
        whole, remaining = sum([portions[i] for i in movable]), spare
        for i in movable:
            extra = min(limit - holding[i], max(1, remaining * portions[i] // whole), spare)
            holding[i] = holding[i] + extra
            spare = spare - extra
    return np.array(holding)


def noise(key, shape, spread, bound, cuts=(), held_as=jnp.bfloat16):
    values = spread * jax.random.normal(key, shape, jnp.float32)
    if cuts:
        values = values * shard_levels(key, shape, cuts, -0.22, 0.18)
    return jnp.clip(values, -bound, bound).astype(held_as)


def setup_inputs(seed: int = 0) -> dict:
    key_of = jax.random.split(jax.random.key(seed), 10)
    entering = noise(key_of[0], (N_PIPE, TOKENS, D), 1.0, 6.0, ((0, 16), (1, 4), (2, 8)))
    pending = noise(key_of[1], (N_PIPE, TOKENS, D), 1.0, 6.0, ((0, 16), (1, 4), (2, 8)))
    stashed_in = noise(key_of[2], (N_PIPE, TOKENS, D), 1.0, 6.0, ((0, 16), (1, 4), (2, 8)))
    forward_routes_keys = jax.random.split(jax.random.fold_in(key_of[3], 1), N_PIPE * TOKENS // TOK)
    forward_routes_turns = jax.random.permutation(jax.random.fold_in(key_of[3], 3), N_PIPE * TOKENS // TOK)
    forward_routes = jax.vmap(lambda own, number: shared_out(jax.random.fold_in(key_of[3], 2), own, number, TOK, EXPERTS, TOPK, CAP, 0))(forward_routes_keys, forward_routes_turns).reshape((N_PIPE, TOKENS, TOPK))
    backward_routes_keys = jax.random.split(jax.random.fold_in(key_of[4], 1), N_PIPE * TOKENS // TOK)
    backward_routes_turns = jax.random.permutation(jax.random.fold_in(key_of[4], 3), N_PIPE * TOKENS // TOK)
    backward_routes = jax.vmap(lambda own, number: shared_out(jax.random.fold_in(key_of[4], 2), own, number, TOK, EXPERTS, TOPK, CAP, 0))(backward_routes_keys, backward_routes_turns).reshape((N_PIPE, TOKENS, TOPK))
    norm_gains = jnp.clip(1.0 + 0.1 * jax.random.normal(key_of[5], (N_PIPE, D), jnp.float32), 0.5, 1.5)
    w_router = noise(key_of[6], (N_PIPE, D, EXPERTS), D ** -0.5, 0.09375, ((0, 16), (1, 8)))
    w_gateup = noise(key_of[7], (N_PIPE, EXPERTS, D, 2, FF), D ** -0.5, 0.09375, ((0, 16), (1, 4), (4, 8)))
    w_down = noise(key_of[8], (N_PIPE, EXPERTS, FF, D), FF ** -0.5, 0.1875, ((0, 16), (1, 4), (2, 8)))
    return dict(entering=entering, pending=pending, stashed_in=stashed_in, forward_routes=forward_routes, backward_routes=backward_routes, norm_gains=norm_gains, w_router=w_router, w_gateup=w_gateup, w_down=w_down)


ROUTE_SCALE = 2.827
EPSILON = 1e-05

def slot_places(routes):
    flattened = routes.reshape(-1).astype(jnp.int32)
    member = (flattened[:, None] == jnp.arange(EXPERTS, dtype=jnp.int32)[None, :]).astype(jnp.int32)
    before = jnp.cumsum(member, axis=0) - member
    position = lax.optimization_barrier(jnp.sum(before * member, axis=1))
    return (flattened * CAP + position).astype(jnp.int32)

def normalize(tokens, gain_row):
    values = tokens.astype(jnp.float32)
    scaling = lax.rsqrt(lax.optimization_barrier(jnp.sum(values * values, axis=-1, keepdims=True)) / D + EPSILON)
    return (values, scaling, (values * scaling * gain_row).astype(jnp.bfloat16))

def gating(moe_in, router, routes):
    logits = jnp.dot(moe_in, router, preferred_element_type=jnp.float32)
    selection = (routes[:, :, None] == jnp.arange(EXPERTS, dtype=jnp.int32)[None, None, :]).astype(jnp.float32)
    chosen = lax.optimization_barrier(jnp.sum(logits[:, None, :] * selection, axis=-1))
    lifted = jax.nn.sigmoid(chosen)
    lifted_sum = lax.optimization_barrier(jnp.sum(lifted, axis=-1, keepdims=True))
    return (ROUTE_SCALE * lifted / lifted_sum, lifted, lifted_sum, selection)

def to_slots(rows, destination):
    filled = jnp.zeros((EXPERTS * CAP, rows.shape[-1]), rows.dtype).at[destination].set(rows)
    return filled.reshape(EXPERTS, CAP, rows.shape[-1])

def grouped_round(partial_value):
    rounded = lax.optimization_barrier(partial_value.astype(jnp.bfloat16))
    return lax.optimization_barrier(jnp.sum(rounded.astype(jnp.float32), axis=-2))

def up_project(buffer, gate_up):
    projected = jnp.einsum('ecd,edkf->eckf', buffer.astype(jnp.float32), gate_up.astype(jnp.float32))
    return (projected[:, :, 0], projected[:, :, 1])

def expert_forward(buffer, gate_up, down_w):
    gate_pre, second = up_project(buffer, gate_up)
    inner_act = (jax.nn.silu(gate_pre) * second).astype(jnp.bfloat16)
    group_width = FF // N_EXPERT
    split_inner = inner_act.reshape(EXPERTS, CAP, N_EXPERT, group_width).astype(jnp.float32)
    split_down = down_w.reshape(EXPERTS, N_EXPERT, group_width, D).astype(jnp.float32)
    partial_value = jnp.einsum('ecgf,egfd->ecgd', split_inner, split_down)
    return grouped_round(partial_value).astype(jnp.bfloat16)

def expert_backward(buffer, upstream, gate_up, down_w):
    gate_pre, second = up_project(buffer, gate_up)
    weighted = jnp.einsum('ecd,efd->ecf', upstream.astype(jnp.float32), down_w.astype(jnp.float32))
    lifted = jax.nn.sigmoid(gate_pre)
    activated = gate_pre * lifted
    inner_act = (activated * second).astype(jnp.bfloat16)
    gate_cot = lax.optimization_barrier(jnp.sum(inner_act.astype(jnp.float32) * weighted, axis=-1)).astype(jnp.bfloat16)
    grad_first = (weighted * second * lifted * (1.0 + gate_pre * (1.0 - lifted))).astype(jnp.bfloat16)
    grad_second = (weighted * activated).astype(jnp.bfloat16)
    stacked = jnp.stack([grad_first, grad_second], axis=2)
    group_width = FF // N_EXPERT
    split_grad = stacked.reshape(EXPERTS, CAP, 2, N_EXPERT, group_width).astype(jnp.float32)
    split_weight = gate_up.reshape(EXPERTS, D, 2, N_EXPERT, group_width).astype(jnp.float32)
    partial_value = jnp.einsum('eckgf,edkgf->ecgd', split_grad, split_weight)
    return (grouped_round(partial_value).astype(jnp.bfloat16), gate_cot)

def layer_forward(tokens, routes, gain_row, router, gate_up, down_w):
    values, scaling, moe_in = normalize(tokens, gain_row)
    gate_weights, lifted, lifted_sum, selection = gating(moe_in, router, routes)
    destination = slot_places(routes)
    buffer = to_slots(jnp.repeat(moe_in, TOPK, axis=0), destination)
    results = expert_forward(buffer, gate_up, down_w).reshape(EXPERTS * CAP, D)
    picked = jnp.take(results, destination, axis=0).reshape(TOK, TOPK, D)
    return (values + lax.optimization_barrier(jnp.sum(gate_weights[:, :, None] * picked.astype(jnp.float32), axis=1))).astype(jnp.bfloat16)

def layer_backward(stashed, incoming, routes, gain_row, router, gate_up, down_w):
    values, scaling, moe_in = normalize(stashed, gain_row)
    gate_weights, lifted, lifted_sum, selection = gating(moe_in, router, routes)
    destination = slot_places(routes)
    buffer = to_slots(jnp.repeat(moe_in, TOPK, axis=0), destination)
    upstream_slots = to_slots(jnp.repeat(incoming, TOPK, axis=0), destination)
    row_cot, gate_cot = expert_backward(buffer, upstream_slots, gate_up, down_w)
    back_rows = jnp.take(row_cot.reshape(EXPERTS * CAP, D), destination, axis=0).reshape(TOK, TOPK, D)
    back_gate = jnp.take(gate_cot.reshape(-1), destination, axis=0).reshape(TOK, TOPK).astype(jnp.float32)
    moe_cot = lax.optimization_barrier(jnp.sum(gate_weights[:, :, None] * back_rows.astype(jnp.float32), axis=1)).astype(jnp.bfloat16)
    mixed = lax.optimization_barrier(jnp.sum(back_gate * lifted, axis=-1, keepdims=True)) / lifted_sum
    chosen_cot = ROUTE_SCALE * (back_gate - mixed) / lifted_sum * lifted * (1.0 - lifted)
    logit_cot = lax.optimization_barrier(jnp.sum(chosen_cot[:, :, None] * selection, axis=1))
    norm_cot = moe_cot.astype(jnp.float32) + jnp.dot(logit_cot, router.astype(jnp.float32).T, precision=lax.Precision.HIGHEST)
    scaled = norm_cot * gain_row
    inner_product = lax.optimization_barrier(jnp.sum(scaled * values, axis=-1, keepdims=True))
    token_cot = incoming.astype(jnp.float32) + scaling * scaled - values * (scaling * scaling * scaling) * inner_product / D
    gain_cot = lax.optimization_barrier(jnp.sum(norm_cot * values * scaling, axis=0))
    return (token_cot.astype(jnp.bfloat16), gain_cot)

def reference(entering, pending, stashed_in, forward_routes, backward_routes, norm_gains, w_router, w_gateup, w_down):
    sequences = TOKENS // TOK

    def section_forward(operands):
        tokens, routes, gain_row, router, gate_up, down_w = operands

        def single(bundle):
            return layer_forward(bundle[0], bundle[1], gain_row, router, gate_up, down_w)
        done = lax.map(single, (tokens.reshape(sequences, TOK, D), routes.reshape(sequences, TOK, TOPK)))
        return done.reshape(TOKENS, D)

    def section_backward(operands):
        stashed, incoming, routes, gain_row, router, gate_up, down_w = operands

        def single(bundle):
            return layer_backward(bundle[0], bundle[1], bundle[2], gain_row, router, gate_up, down_w)
        cotangents, gain_parts = lax.map(single, (stashed.reshape(sequences, TOK, D), incoming.reshape(sequences, TOK, D), routes.reshape(sequences, TOK, TOPK)))
        return (cotangents.reshape(TOKENS, D), lax.optimization_barrier(jnp.sum(gain_parts, axis=0)))
    produced = lax.map(section_forward, (entering, forward_routes, norm_gains, w_router, w_gateup, w_down))
    cotangents, gain_grads = lax.map(section_backward, (stashed_in, pending, backward_routes, norm_gains, w_router, w_gateup, w_down))
    passed_forward = jnp.concatenate([jnp.zeros_like(produced[:1]), produced[:-1]], axis=0)
    passed_backward = jnp.concatenate([cotangents[1:], jnp.zeros_like(cotangents[:1])], axis=0)
    return (produced, cotangents, passed_forward, passed_backward, gain_grads)
```

```python
import jax
import jax.numpy as jnp
from jax import lax
from jax.sharding import PartitionSpec as P

D = 4096
ROUTE_SCALE = 2.827
EPSILON = 1e-05
F32 = jnp.float32
BF16 = jnp.bfloat16


def summed_over(values, axis):
    copies = jnp.broadcast_to(values, (lax.axis_size(axis), *values.shape))
    return jnp.sum(lax.all_to_all(copies, axis, split_axis=0, concat_axis=0, tiled=True), axis=0)


def exchanged(blocks, axis):
    return lax.all_to_all(blocks, axis, split_axis=0, concat_axis=0, tiled=True)


def shifted(block, axis, distance):
    devices = range(lax.axis_size(axis))
    route = [(i - distance, i) for i in devices if i - distance in devices]
    return lax.ppermute(block, axis, route)


def slots_of(routes, experts, capacity):
    length = routes.shape[0]
    names = routes.T
    member = (names[:, None, :] == jnp.arange(experts, dtype=jnp.int32)[None, :, None]).astype(F32)
    token = jnp.arange(length, dtype=jnp.int32)
    earlier = (token[:, None] < token[None, :]).astype(BF16)
    before = jnp.dot(
        jnp.sum(member, axis=0).astype(BF16), earlier, preferred_element_type=F32
    )
    position = jnp.sum(member * before[None], axis=1).astype(jnp.int32)
    slot = names * capacity + position
    every = jnp.arange(experts * capacity, dtype=jnp.int32)
    placed = slot[:, None, :] == every[None, :, None]
    return slot, placed, member


def gates_of(squares, raw_logits, member):
    scaling = lax.rsqrt(squares / D + EPSILON)
    chosen = jnp.sum(member * raw_logits[None], axis=1) * scaling[None]
    lifted = jax.nn.sigmoid(chosen)
    lifted_sum = jnp.sum(lifted, axis=0, keepdims=True)
    return scaling, chosen, lifted, lifted_sum, ROUTE_SCALE * lifted / lifted_sum


def split_three(values):
    high = values.astype(BF16)
    rest = values - high.astype(F32)
    middle = rest.astype(BF16)
    low = (rest - middle.astype(F32)).astype(BF16)
    return high, middle, low


def local(
    entering,
    pending,
    stashed_in,
    forward_routes,
    backward_routes,
    norm_gains,
    w_router,
    w_gateup,
    w_down,
):
    gain = norm_gains[0]
    router = w_router[0]
    gate_up = w_gateup[0, 0].reshape(D, -1)
    down_w = w_down[0, 0]
    hidden = down_w.shape[0]
    tokens, stashed, incoming = entering[0], stashed_in[0], pending[0]
    length, width = tokens.shape
    experts = router.shape[1]
    capacity = length * forward_routes.shape[2] // experts

    slot_f, placed_f, member_f = slots_of(forward_routes[0], experts, capacity)
    slot_b, placed_b, member_b = slots_of(backward_routes[0], experts, capacity)
    spread_f = (placed_f[0] | placed_f[1]).astype(BF16)
    spread_b = (placed_b[0] | placed_b[1]).astype(BF16)
    tokens32, stashed32 = tokens.astype(F32), stashed.astype(F32)
    scaled_f = (tokens32 * gain).astype(BF16)
    scaled_b = (stashed32 * gain).astype(BF16)

    def routed(spread, rows):
        return jnp.dot(spread, rows, preferred_element_type=F32).astype(BF16).reshape(
            experts, capacity, width
        )

    sent = jnp.concatenate(
        [routed(spread_f, scaled_f), routed(spread_b, scaled_b), routed(spread_b, incoming)], axis=1
    )
    arrived = exchanged(sent, "dp").reshape(experts, 3, capacity, width)
    slots = experts * capacity
    arrived = arrived.transpose(1, 0, 2, 3).reshape(3 * slots, width)
    whole = lax.all_gather(arrived, "expert", axis=1, tiled=True)

    (scaled_f2, scaled_b2), arrived2 = lax.optimization_barrier(((scaled_f, scaled_b), arrived))

    def sums_of(values32, scaled):
        squares = jnp.sum(values32 * values32, axis=-1)[None]
        logits = lax.dot_general(
            router, scaled, (((0,), (1,)), ((), ())), preferred_element_type=F32
        )
        return [squares, logits]

    sums = jnp.concatenate(
        sums_of(tokens32, scaled_f2)
        + sums_of(stashed32, scaled_b2)
        + [jnp.zeros((16 - 2 * (experts + 1), length), F32)],
        axis=0,
    )
    sums = summed_over(sums, "expert")
    r_f, _, _, _, gates_f = gates_of(sums[0], sums[1 : 1 + experts], member_f)
    r_b, chosen_b, lifted_b, lifted_sum_b, gates_b = gates_of(
        sums[1 + experts], sums[2 + experts : 2 + 2 * experts], member_b
    )

    def by_slot(placed, values):
        return jnp.sum(jnp.where(placed, values[:, None, :], 0.0), axis=(0, 2))

    twice = lambda v: jnp.broadcast_to(v[None], (2, length))
    scalars = jnp.stack(
        [
            by_slot(placed_f, twice(r_f)),
            by_slot(placed_f, gates_f),
            by_slot(placed_b, twice(r_b)),
            by_slot(placed_b, gates_b),
        ]
    )
    scalars = exchanged(scalars.reshape(4, experts, capacity).transpose(1, 0, 2), "dp")
    scalars = scalars.transpose(1, 0, 2).reshape(4, slots)
    row_r = jnp.concatenate([scalars[0], scalars[2]])[:, None]
    row_gate_f, row_r_b, row_gate_b = scalars[1][:, None], scalars[2][:, None], scalars[3][:, None]

    whole, row_r = lax.optimization_barrier((whole, row_r))
    projected = jnp.dot(whole[: 2 * slots], gate_up, preferred_element_type=F32) * row_r
    first, second = projected[:, :hidden], projected[:, hidden:]
    lifted_act = jax.nn.sigmoid(first)
    activated = first * lifted_act
    inner = (activated * second).astype(BF16)
    out_f = jnp.dot(inner[:slots], down_w, preferred_element_type=F32) * row_gate_f
    first, second = first[slots:], second[slots:]
    lifted_act, activated = lifted_act[slots:], activated[slots:]
    weighted = lax.dot_general(
        whole[2 * slots :], down_w, (((1,), (1,)), ((), ())), preferred_element_type=F32
    )
    gate_part = jnp.sum(inner[slots:].astype(F32) * weighted, axis=1)
    grad_first = (weighted * second * lifted_act * (1.0 + first * (1.0 - lifted_act))).astype(BF16)
    grad_second = (weighted * activated).astype(BF16)
    along_part = jnp.sum(
        grad_first.astype(F32) * first + grad_second.astype(F32) * second, axis=1
    )
    grads = jnp.concatenate([grad_first, grad_second], axis=1)
    out_b = (
        lax.dot_general(grads, gate_up, (((1,), (1,)), ((), ())), preferred_element_type=F32)
        * row_gate_b
    )
    partial = jnp.concatenate([out_f.astype(BF16), out_b.astype(BF16)], axis=0)
    summed = lax.psum_scatter(partial, "expert", scatter_dimension=1, tiled=True)

    parts = jnp.stack([gate_part, along_part])
    (parts, _) = lax.optimization_barrier((parts, partial))
    parts = summed_over(parts, "expert")
    parts = exchanged(parts.reshape(2, experts, capacity).transpose(1, 0, 2), "dp")
    parts = parts.transpose(1, 0, 2).reshape(2, slots)

    def by_token(values):
        return jnp.sum(jnp.where(placed_b, values[None, :, None], 0.0), axis=1)

    back_gate = by_token(parts[0].astype(BF16).astype(F32))
    along = by_token(parts[1])
    mixed = jnp.sum(back_gate * lifted_b, axis=0, keepdims=True) / lifted_sum_b
    chosen_cot = ROUTE_SCALE * (back_gate - mixed) / lifted_sum_b * lifted_b * (1.0 - lifted_b)
    logit_cot = jnp.sum(member_b * chosen_cot[:, None, :], axis=0)
    inner_r = jnp.sum(gates_b * along + chosen_cot * chosen_b, axis=0)
    router_part = lax.dot_general(
        logit_cot,
        router.astype(F32),
        (((0,), (1,)), ((), ())),
        precision=lax.Precision.HIGHEST,
        preferred_element_type=F32,
    )
    own_gain = jnp.sum(router_part * stashed32 * r_b[:, None], axis=0)
    base = (
        incoming.astype(F32)
        + (r_b[:, None] * router_part) * gain
        - stashed32 * (r_b * r_b * inner_r / D)[:, None]
    )

    gain_part = own_gain + (
        jnp.sum(
            summed[slots:].astype(F32) * arrived2[slots : 2 * slots].astype(F32) * row_r_b, axis=0
        )
        / gain
    )
    extra = jnp.concatenate(
        [v[None] for v in split_three(gain_part)] + [jnp.zeros((5, width), BF16)], axis=0
    )
    back = jnp.concatenate(
        [
            summed[:slots].reshape(experts, capacity, width),
            summed[slots:].reshape(experts, capacity, width),
            jnp.broadcast_to(extra[None], (experts, 8, width)),
        ],
        axis=1,
    )
    back = exchanged(back, "dp")

    def gathered(spread, rows):
        return lax.dot_general(
            spread,
            rows.reshape(slots, width),
            (((0,), (0,)), ((), ())),
            preferred_element_type=F32,
        )

    produced = (tokens32 + gathered(spread_f, back[:, :capacity])).astype(BF16)
    passed_forward = shifted(produced, "pipe", 1)
    moe_cot = gathered(spread_b, back[:, capacity : 2 * capacity])
    cotangent = (base + (r_b[:, None] * moe_cot) * gain).astype(BF16)
    passed_backward = shifted(cotangent, "pipe", -1)
    gain_total = jnp.sum(back[:, 2 * capacity : 2 * capacity + 3].astype(F32), axis=(0, 1))
    return (
        produced[None],
        cotangent[None],
        passed_forward[None],
        passed_backward[None],
        gain_total[None],
    )


def solution(mesh):
    placed = (
        P("pipe", "dp", "expert"),
        P("pipe", "dp", "expert"),
        P("pipe", "dp", "expert"),
        P("pipe", "dp", None),
        P("pipe", "dp", None),
        P("pipe", "expert"),
        P("pipe", "expert", None),
        P("pipe", "dp", None, None, "expert"),
        P("pipe", "dp", "expert", None),
    )
    return jax.shard_map(
        local,
        mesh=mesh,
        in_specs=placed,
        out_specs=(
            P("pipe", "dp", "expert"),
            P("pipe", "dp", "expert"),
            P("pipe", "dp", "expert"),
            P("pipe", "dp", "expert"),
            P("pipe", "expert"),
        ),
        check_vma=False,
    )
```

```python
import jax
import jax.numpy as jnp
from jax import lax
from jax.experimental import pallas as pl
from jax.experimental.pallas import tpu as pltpu
from jax.sharding import PartitionSpec as P

D = 4096
ROUTE_SCALE = 2.827
EPSILON = 1e-05
F32 = jnp.float32
BF16 = jnp.bfloat16


def summed_over(values, axis):
    copies = jnp.broadcast_to(values, (lax.axis_size(axis), *values.shape))
    return jnp.sum(lax.all_to_all(copies, axis, split_axis=0, concat_axis=0, tiled=True), axis=0)


def exchanged(blocks, axis):
    return lax.all_to_all(blocks, axis, split_axis=0, concat_axis=0, tiled=True)


def shifted(block, axis, distance):
    devices = range(lax.axis_size(axis))
    route = [(i - distance, i) for i in devices if i - distance in devices]
    return lax.ppermute(block, axis, route)


def rotated(block, axis, distance):
    size = lax.axis_size(axis)
    return lax.ppermute(block, axis, [(i, (i + distance) % size) for i in range(size)])


def slots_of(routes, experts, capacity):
    length = routes.shape[0]
    names = routes.T
    member = (names[:, None, :] == jnp.arange(experts, dtype=jnp.int32)[None, :, None]).astype(F32)
    token = jnp.arange(length, dtype=jnp.int32)
    earlier = (token[:, None] < token[None, :]).astype(BF16)
    before = jnp.dot(
        jnp.sum(member, axis=0).astype(BF16), earlier, preferred_element_type=F32
    )
    position = jnp.sum(member * before[None], axis=1).astype(jnp.int32)
    slot = names * capacity + position
    every = jnp.arange(experts * capacity, dtype=jnp.int32)
    placed = slot[:, None, :] == every[None, :, None]
    return slot, placed, member


def gates_of(squares, raw_logits, member):
    scaling = lax.rsqrt(squares / D + EPSILON)
    chosen = jnp.sum(member * raw_logits[None], axis=1) * scaling[None]
    lifted = jax.nn.sigmoid(chosen)
    lifted_sum = jnp.sum(lifted, axis=0, keepdims=True)
    return scaling, chosen, lifted, lifted_sum, ROUTE_SCALE * lifted / lifted_sum


def dispatch_kernel(routes_f, routes_b, gain, tokens, stashed, incoming, sent):
    experts, _, width = sent.shape
    length = tokens.shape[0]
    capacity = sent.shape[1] // 3
    shape = (2 * experts, length)
    row = lax.broadcasted_iota(jnp.int32, shape, 0)
    forward = row < experts
    expert = jnp.where(forward, row, row - experts)

    def named(k):
        return (
            jnp.where(
                forward,
                jnp.broadcast_to(routes_f[k : k + 1, :], shape),
                jnp.broadcast_to(routes_b[k : k + 1, :], shape),
            )
            == expert
        )

    member = named(0) | named(1)
    square = (length, length)
    earlier = jnp.where(
        lax.broadcasted_iota(jnp.int32, square, 0) < lax.broadcasted_iota(jnp.int32, square, 1),
        1.0,
        0.0,
    ).astype(BF16)
    before = jnp.dot(
        jnp.where(member, 1.0, 0.0).astype(BF16), earlier, preferred_element_type=F32
    )
    place = jnp.where(member, before.astype(jnp.int32), -1)
    slot = lax.broadcasted_iota(jnp.int32, (capacity, length), 0)

    def spread(first):
        return jnp.concatenate(
            [
                jnp.where(slot == place[e : e + 1, :], 1.0, 0.0).astype(BF16)
                for e in range(first, first + experts)
            ],
            axis=0,
        )

    spread_f, spread_b = spread(0), spread(experts)
    scaled_f = (tokens[...].astype(F32) * gain[...]).astype(BF16)
    scaled_b = (stashed[...].astype(F32) * gain[...]).astype(BF16)
    for k, (moved, rows) in enumerate(
        ((spread_f, scaled_f), (spread_b, scaled_b), (spread_b, incoming[...]))
    ):
        routed = jnp.dot(moved, rows, preferred_element_type=F32).astype(BF16)
        for e in range(experts):
            sent[e, k * capacity : (k + 1) * capacity, :] = routed[
                e * capacity : (e + 1) * capacity
            ]


def expert_kernel(
    whole, gate_up, down_w, row_r, row_gate, partial, gate_part, along_part, rows, outs, sums, took, left
):
    pieces, experts, _, width = whole.shape
    capacity = whole.shape[2] // 3
    slots = experts * capacity
    hidden = down_w.shape[0]

    def fetch(z, k):
        return pltpu.make_async_copy(
            whole.at[z, :, pl.ds(k * capacity, capacity), :], rows.at[z, k], took.at[z, k]
        )

    def put(z, k):
        return pltpu.make_async_copy(
            outs.at[z, k], partial.at[z, :, pl.ds(k * capacity, capacity), :], left.at[z, k]
        )

    for z in range(pieces):
        for k in range(3):
            fetch(z, k).start()
    weighted = None
    for z in range(pieces):
        part = slice(z * width, (z + 1) * width)
        for k in range(3):
            fetch(z, k).wait()
        values = rows[z, 0:2].reshape(2 * slots, width)
        product = jnp.dot(values, gate_up[part, :], preferred_element_type=F32)
        incoming = rows[z, 2].reshape(slots, width)
        product_w = lax.dot_general(
            incoming, down_w[:, part], (((1,), (1,)), ((), ())), preferred_element_type=F32
        )
        if z == 0:
            sums[...] = product
            weighted = product_w
        else:
            sums[...] += product
            weighted += product_w
    first = sums[:, :hidden] * row_r[...]
    second = sums[:, hidden:] * row_r[...]
    lifted = jax.nn.sigmoid(first)
    activated = first * lifted
    inner = (activated * second).astype(BF16)
    inner_f = inner[:slots]
    first, second, lifted, activated = first[slots:], second[slots:], lifted[slots:], activated[slots:]
    gate_part[...] = jnp.sum(inner[slots:].astype(F32) * weighted, axis=1, keepdims=True)
    grad_first = (weighted * second * lifted * (1.0 + first * (1.0 - lifted))).astype(BF16)
    grad_second = (weighted * activated).astype(BF16)
    along_part[...] = jnp.sum(
        grad_first.astype(F32) * first + grad_second.astype(F32) * second, axis=1, keepdims=True
    )
    grads = jnp.concatenate([grad_first, grad_second], axis=1)
    gate_f, gate_b = row_gate[:slots], row_gate[slots:]
    for z in range(pieces):
        part = slice(z * width, (z + 1) * width)
        out_f = jnp.dot(inner_f, down_w[:, part], preferred_element_type=F32) * gate_f
        outs[z, 0] = out_f.astype(BF16).reshape(experts, capacity, width)
        put(z, 0).start()
        out_b = (
            lax.dot_general(
                grads, gate_up[part, :], (((1,), (1,)), ((), ())), preferred_element_type=F32
            )
            * gate_b
        )
        outs[z, 1] = out_b.astype(BF16).reshape(experts, capacity, width)
        put(z, 1).start()
    for z in range(pieces):
        for k in range(2):
            put(z, k).wait()


def local(
    entering,
    pending,
    stashed_in,
    forward_routes,
    backward_routes,
    norm_gains,
    w_router,
    w_gateup,
    w_down,
):
    gain = norm_gains[0]
    router = w_router[0]
    gate_up = w_gateup[0, 0].reshape(D, -1)
    down_w = w_down[0, 0]
    hidden = down_w.shape[0]
    tokens, stashed, incoming = entering[0], stashed_in[0], pending[0]
    length, width = tokens.shape
    experts = router.shape[1]
    capacity = length * forward_routes.shape[2] // experts

    slots = experts * capacity
    pieces = lax.axis_size("expert")
    vmem = pl.BlockSpec(memory_space=pltpu.VMEM)
    hbm = pl.BlockSpec(memory_space=pl.ANY)
    sent = pl.pallas_call(
        dispatch_kernel,
        out_shape=jax.ShapeDtypeStruct((experts, 3 * capacity, width), BF16),
        in_specs=[vmem] * 6,
        out_specs=vmem,
    )(
        forward_routes[0].T,
        backward_routes[0].T,
        gain[None],
        tokens,
        stashed,
        incoming,
    )
    arrived = exchanged(sent, "dp")
    whole = lax.all_gather(arrived.reshape(3 * slots, width), "expert", axis=0, tiled=True)

    (tokens, stashed, incoming, gain, routes_f, routes_b), arrived2 = lax.optimization_barrier(
        ((tokens, stashed, incoming, gain, forward_routes[0], backward_routes[0]), arrived)
    )
    slot_f, placed_f, member_f = slots_of(routes_f, experts, capacity)
    slot_b, placed_b, member_b = slots_of(routes_b, experts, capacity)
    spread_f = (placed_f[0] | placed_f[1]).astype(BF16)
    spread_b = (placed_b[0] | placed_b[1]).astype(BF16)
    tokens32, stashed32 = tokens.astype(F32), stashed.astype(F32)
    scaled_f2 = (tokens32 * gain).astype(BF16)
    scaled_b2 = (stashed32 * gain).astype(BF16)

    def sums_of(values32, scaled):
        squares = jnp.sum(values32 * values32, axis=-1)[None]
        logits = lax.dot_general(
            router, scaled, (((0,), (1,)), ((), ())), preferred_element_type=F32
        )
        return [squares, logits]

    sums = jnp.concatenate(
        sums_of(tokens32, scaled_f2)
        + sums_of(stashed32, scaled_b2)
        + [jnp.zeros((16 - 2 * (experts + 1), length), F32)],
        axis=0,
    )
    sums = summed_over(sums, "expert")
    r_f, _, _, _, gates_f = gates_of(sums[0], sums[1 : 1 + experts], member_f)
    r_b, chosen_b, lifted_b, lifted_sum_b, gates_b = gates_of(
        sums[1 + experts], sums[2 + experts : 2 + 2 * experts], member_b
    )

    def by_slot(placed, values):
        return jnp.sum(jnp.where(placed, values[:, None, :], 0.0), axis=(0, 2))

    twice = lambda v: jnp.broadcast_to(v[None], (2, length))
    scalars = jnp.stack(
        [
            by_slot(placed_f, twice(r_f)),
            by_slot(placed_f, gates_f),
            by_slot(placed_b, twice(r_b)),
            by_slot(placed_b, gates_b),
        ]
    )
    scalars = exchanged(scalars.reshape(4, experts, capacity).transpose(1, 0, 2), "dp")
    scalars = scalars.transpose(1, 0, 2).reshape(4, slots)
    row_r = jnp.concatenate([scalars[0], scalars[2]])[:, None]
    row_gate = jnp.concatenate([scalars[1], scalars[3]])[:, None]
    row_r_b = scalars[2].reshape(experts, capacity, 1)

    partial, gate_part, along_part = pl.pallas_call(
        expert_kernel,
        out_shape=(
            jax.ShapeDtypeStruct((pieces, experts, 2 * capacity, width), BF16),
            jax.ShapeDtypeStruct((slots, 1), F32),
            jax.ShapeDtypeStruct((slots, 1), F32),
        ),
        in_specs=[hbm] + [vmem] * 4,
        out_specs=(hbm, vmem, vmem),
        scratch_shapes=[
            pltpu.VMEM((pieces, 3, experts, capacity, width), BF16),
            pltpu.VMEM((pieces, 2, experts, capacity, width), BF16),
            pltpu.VMEM((2 * slots, 2 * hidden), F32),
            pltpu.SemaphoreType.DMA((pieces, 3)),
            pltpu.SemaphoreType.DMA((pieces, 2)),
        ],
    )(whole.reshape(pieces, experts, 3 * capacity, width), gate_up, down_w, row_r, row_gate)
    summed = lax.psum_scatter(
        partial.reshape(pieces * 2 * slots, width), "expert", scatter_dimension=0, tiled=True
    )
    summed = summed.reshape(experts, 2 * capacity, width)

    parts = jnp.stack([gate_part[:, 0], along_part[:, 0]])
    parts = summed_over(parts, "expert")
    parts = exchanged(parts.reshape(2, experts, capacity).transpose(1, 0, 2), "dp")
    parts = parts.transpose(1, 0, 2).reshape(2, slots)

    def by_token(values):
        return jnp.sum(jnp.where(placed_b, values[None, :, None], 0.0), axis=1)

    back_gate = by_token(parts[0].astype(BF16).astype(F32))
    along = by_token(parts[1])
    mixed = jnp.sum(back_gate * lifted_b, axis=0, keepdims=True) / lifted_sum_b
    chosen_cot = ROUTE_SCALE * (back_gate - mixed) / lifted_sum_b * lifted_b * (1.0 - lifted_b)
    logit_cot = jnp.sum(member_b * chosen_cot[:, None, :], axis=0)
    inner_r = jnp.sum(gates_b * along + chosen_cot * chosen_b, axis=0)
    router_part = lax.dot_general(
        logit_cot,
        router.astype(F32),
        (((0,), (1,)), ((), ())),
        precision=lax.Precision.HIGHEST,
        preferred_element_type=F32,
    )
    own_gain = jnp.sum(router_part * stashed32 * r_b[:, None], axis=0)
    base = (
        incoming.astype(F32)
        + (r_b[:, None] * router_part) * gain
        - stashed32 * (r_b * r_b * inner_r / D)[:, None]
    )

    back = exchanged(summed, "dp")
    gain_part = own_gain + (
        jnp.sum(
            summed[:, capacity:].astype(F32)
            * arrived2[:, capacity : 2 * capacity].astype(F32)
            * row_r_b,
            axis=(0, 1),
        )
        / gain
    )
    others = [rotated(gain_part[None], "dp", distance) for distance in range(1, experts)]
    back, others = lax.optimization_barrier((back, others))
    gain_total = gain_part + sum(other[0] for other in others)

    def gathered(spread, rows):
        return lax.dot_general(
            spread,
            rows.reshape(slots, width),
            (((0,), (0,)), ((), ())),
            preferred_element_type=F32,
        )

    produced = (tokens32 + gathered(spread_f, back[:, :capacity])).astype(BF16)
    passed_forward = shifted(produced, "pipe", 1)
    moe_cot = gathered(spread_b, back[:, capacity : 2 * capacity])
    cotangent = (base + (r_b[:, None] * moe_cot) * gain).astype(BF16)
    passed_backward = shifted(cotangent, "pipe", -1)
    return (
        produced[None],
        cotangent[None],
        passed_forward[None],
        passed_backward[None],
        gain_total[None],
    )


def solution(mesh):
    placed = (
        P("pipe", "dp", "expert"),
        P("pipe", "dp", "expert"),
        P("pipe", "dp", "expert"),
        P("pipe", "dp", None),
        P("pipe", "dp", None),
        P("pipe", "expert"),
        P("pipe", "expert", None),
        P("pipe", "dp", None, None, "expert"),
        P("pipe", "dp", "expert", None),
    )
    return jax.shard_map(
        local,
        mesh=mesh,
        in_specs=placed,
        out_specs=(
            P("pipe", "dp", "expert"),
            P("pipe", "dp", "expert"),
            P("pipe", "dp", "expert"),
            P("pipe", "dp", "expert"),
            P("pipe", "expert"),
        ),
        check_vma=False,
    )
```

```python
import functools

import jax
import jax.numpy as jnp
from jax import lax
from jax.experimental import pallas as pl
from jax.experimental.pallas import tpu as pltpu
from jax.sharding import PartitionSpec as P


D = 4096
ROUTE_SCALE = 2.827
EPSILON = 1e-05
F32 = jnp.float32
BF16 = jnp.bfloat16


def summed_over(values, axis):
    copies = jnp.broadcast_to(values, (lax.axis_size(axis), *values.shape))
    return jnp.sum(lax.all_to_all(copies, axis, split_axis=0, concat_axis=0, tiled=True), axis=0)


def exchanged(blocks, axis):
    return lax.all_to_all(blocks, axis, split_axis=0, concat_axis=0, tiled=True)


def shifted(block, axis, distance):
    devices = range(lax.axis_size(axis))
    route = [(i - distance, i) for i in devices if i - distance in devices]
    return lax.ppermute(block, axis, route)


def rotated(block, axis, distance):
    size = lax.axis_size(axis)
    return lax.ppermute(block, axis, [(i, (i + distance) % size) for i in range(size)])


def slots_of(routes, experts, capacity):
    length = routes.shape[0]
    names = routes.T
    member = (names[:, None, :] == jnp.arange(experts, dtype=jnp.int32)[None, :, None]).astype(F32)
    token = jnp.arange(length, dtype=jnp.int32)
    earlier = (token[:, None] < token[None, :]).astype(BF16)
    before = jnp.dot(
        jnp.sum(member, axis=0).astype(BF16), earlier, preferred_element_type=F32
    )
    position = jnp.sum(member * before[None], axis=1).astype(jnp.int32)
    slot = names * capacity + position
    every = jnp.arange(experts * capacity, dtype=jnp.int32)
    placed = slot[:, None, :] == every[None, :, None]
    return slot, placed, member


def gates_of(squares, raw_logits, member):
    scaling = lax.rsqrt(squares / D + EPSILON)
    chosen = jnp.sum(member * raw_logits[None], axis=1) * scaling[None]
    lifted = jax.nn.sigmoid(chosen)
    lifted_sum = jnp.sum(lifted, axis=0, keepdims=True)
    return scaling, chosen, lifted, lifted_sum, ROUTE_SCALE * lifted / lifted_sum


def dispatch_kernel(routes_f, routes_b, gain, tokens, stashed, incoming, sent):
    experts, _, _ = sent.shape
    length = tokens.shape[0]
    capacity = sent.shape[1] // 3
    shape = (2 * experts, length)
    row = lax.broadcasted_iota(jnp.int32, shape, 0)
    forward = row < experts
    expert = jnp.where(forward, row, row - experts)

    def named(k):
        return (
            jnp.where(
                forward,
                jnp.broadcast_to(routes_f[k : k + 1, :], shape),
                jnp.broadcast_to(routes_b[k : k + 1, :], shape),
            )
            == expert
        )

    member = named(0) | named(1)
    square = (length, length)
    earlier = jnp.where(
        lax.broadcasted_iota(jnp.int32, square, 0) < lax.broadcasted_iota(jnp.int32, square, 1),
        1.0,
        0.0,
    ).astype(BF16)
    before = jnp.dot(
        jnp.where(member, 1.0, 0.0).astype(BF16), earlier, preferred_element_type=F32
    )
    place = jnp.where(member, before.astype(jnp.int32), -1)
    slot = lax.broadcasted_iota(jnp.int32, (capacity, length), 0)

    def spread(first):
        return jnp.concatenate(
            [
                jnp.where(slot == place[e : e + 1, :], 1.0, 0.0).astype(BF16)
                for e in range(first, first + experts)
            ],
            axis=0,
        )

    spread_f, spread_b = spread(0), spread(experts)
    scaled_f = (tokens[...].astype(F32) * gain[...]).astype(BF16)
    scaled_b = (stashed[...].astype(F32) * gain[...]).astype(BF16)
    for k, (moved, rows) in enumerate(
        ((spread_f, scaled_f), (spread_b, scaled_b), (spread_b, incoming[...]))
    ):
        routed = jnp.dot(moved, rows, preferred_element_type=F32).astype(BF16)
        for e in range(experts):
            sent[e, k * capacity : (k + 1) * capacity, :] = routed[
                e * capacity : (e + 1) * capacity
            ]


def expert_kernel(pieces, at, gate_up, down_w, row_r, row_gate, *refs):
    arrived, refs = refs[: 2 * pieces], refs[2 * pieces :]
    partial, refs = refs[: 2 * pieces], refs[2 * pieces :]
    gate_part, along_part, gain_part, sums = refs
    half, rows, width = arrived[0].shape
    capacity = rows // 3
    part_rows = half * capacity
    slots = 2 * part_rows
    hidden = down_w.shape[0]

    def start(j):
        return pl.multiple_of(((at[0] + j) % pieces) * width, width)

    def taken(j, k):
        return [
            arrived[2 * j + c][:, k * capacity : (k + 1) * capacity, :].reshape(part_rows, width)
            for c in range(2)
        ]

    weighted = None
    for j in range(pieces):
        values = jnp.concatenate(taken(j, 0) + taken(j, 1), axis=0)
        product = jnp.dot(
            values, gate_up[pl.ds(start(j), width), :], preferred_element_type=F32
        )
        product_w = lax.dot_general(
            jnp.concatenate(taken(j, 2), axis=0),
            down_w[:, pl.ds(start(j), width)],
            (((1,), (1,)), ((), ())),
            preferred_element_type=F32,
        )
        if j == 0:
            sums[...] = product
            weighted = product_w
        else:
            sums[...] += product
            weighted += product_w
    first = sums[:, :hidden] * row_r[...]
    second = sums[:, hidden:] * row_r[...]
    lifted = jax.nn.sigmoid(first)
    activated = first * lifted
    inner = (activated * second).astype(BF16)
    inner_f = inner[:slots]
    first, second, lifted, activated = first[slots:], second[slots:], lifted[slots:], activated[slots:]
    gate_part[...] = jnp.sum(inner[slots:].astype(F32) * weighted, axis=1, keepdims=True)
    grad_first = (weighted * second * lifted * (1.0 + first * (1.0 - lifted))).astype(BF16)
    grad_second = (weighted * activated).astype(BF16)
    along_part[...] = jnp.sum(
        grad_first.astype(F32) * first + grad_second.astype(F32) * second, axis=1, keepdims=True
    )
    grads = jnp.concatenate([grad_first, grad_second], axis=1)
    gate_f, gate_b, r_b = row_gate[:slots], row_gate[slots:], row_r[slots:]
    for j in range(pieces):
        out_f = (
            jnp.dot(inner_f, down_w[:, pl.ds(start(j), width)], preferred_element_type=F32) * gate_f
        )
        out_b = (
            lax.dot_general(
                grads,
                gate_up[pl.ds(start(j), width), :],
                (((1,), (1,)), ((), ())),
                preferred_element_type=F32,
            )
            * gate_b
        )
        stashed = jnp.concatenate(taken(j, 1), axis=0).astype(F32)
        gain_part[j : j + 1, :] = jnp.sum(out_b * r_b * stashed, axis=0, keepdims=True)
        for k, out in enumerate((out_f.astype(BF16), out_b.astype(BF16))):
            for c in range(2):
                partial[2 * j + c][:, k * capacity : (k + 1) * capacity, :] = out[
                    c * part_rows : (c + 1) * part_rows
                ].reshape(half, capacity, width)


def ring_gather(first, second, axis):
    size = lax.axis_size(axis)
    middle = size // 2
    found = [[None, None] for _ in range(size)]
    found[0] = [first, second]
    for step in range(1, middle):
        for c in range(2):
            found[size - step][c] = rotated(found[(size - step + 1) % size][c], axis, 1)
            found[step][c] = rotated(found[step - 1][c], axis, -1)
    found[middle][0] = rotated(found[middle + 1][0], axis, 1)
    found[middle][1] = rotated(found[middle - 1][1], axis, -1)
    return [block for pair in found for block in pair]


def ring_scatter(parts, axis):
    size = lax.axis_size(axis)
    middle = size // 2

    def plus(a, b):
        return (a.astype(F32) + b.astype(F32)).astype(BF16)

    def passed(come, mine, distance):
        return rotated(mine if come is None else plus(come, mine), axis, distance)

    up = [passed(None, parts[2 * middle], 1), None]
    down = [None, passed(None, parts[2 * middle + 1], -1)]
    for turn in range(1, middle):
        step = middle - turn
        for c in range(2):
            up[c] = passed(up[c], parts[2 * step + c], 1)
            down[c] = passed(down[c], parts[2 * (size - step) + c], -1)
    return [
        (parts[c].astype(F32) + up[c].astype(F32) + down[c].astype(F32)).astype(BF16)
        for c in range(2)
    ]


def local(
    entering,
    pending,
    stashed_in,
    forward_routes,
    backward_routes,
    norm_gains,
    w_router,
    w_gateup,
    w_down,
):
    gain = norm_gains[0]
    router = w_router[0]
    gate_up = w_gateup[0, 0].reshape(D, -1)
    down_w = w_down[0, 0]
    hidden = down_w.shape[0]
    tokens, stashed, incoming = entering[0], stashed_in[0], pending[0]
    length, width = tokens.shape
    experts = router.shape[1]
    capacity = length * forward_routes.shape[2] // experts

    slots = experts * capacity
    pieces = lax.axis_size("expert")
    vmem = pl.BlockSpec(memory_space=pltpu.VMEM)
    sent = pl.pallas_call(
        dispatch_kernel,
        out_shape=jax.ShapeDtypeStruct((experts, 3 * capacity, width), BF16),
        in_specs=[vmem] * 6,
        out_specs=vmem,
    )(
        forward_routes[0].T,
        backward_routes[0].T,
        gain[None],
        tokens,
        stashed,
        incoming,
    )
    arrived = exchanged(sent, "dp")
    whole = ring_gather(arrived[: experts // 2], arrived[experts // 2 :], "expert")

    (tokens, stashed, incoming, gain, routes_f, routes_b), _ = lax.optimization_barrier(
        ((tokens, stashed, incoming, gain, forward_routes[0], backward_routes[0]), arrived)
    )
    _, placed_f, member_f = slots_of(routes_f, experts, capacity)
    _, placed_b, member_b = slots_of(routes_b, experts, capacity)
    spread_f = (placed_f[0] | placed_f[1]).astype(BF16)
    spread_b = (placed_b[0] | placed_b[1]).astype(BF16)
    tokens32, stashed32 = tokens.astype(F32), stashed.astype(F32)
    scaled_f2 = (tokens32 * gain).astype(BF16)
    scaled_b2 = (stashed32 * gain).astype(BF16)

    def sums_of(values32, scaled):
        squares = jnp.sum(values32 * values32, axis=-1)[None]
        logits = lax.dot_general(
            router, scaled, (((0,), (1,)), ((), ())), preferred_element_type=F32
        )
        return [squares, logits]

    sums = jnp.concatenate(
        sums_of(tokens32, scaled_f2)
        + sums_of(stashed32, scaled_b2)
        + [jnp.zeros((16 - 2 * (experts + 1), length), F32)],
        axis=0,
    )
    sums = summed_over(sums, "expert")
    r_f, _, _, _, gates_f = gates_of(sums[0], sums[1 : 1 + experts], member_f)
    r_b, chosen_b, lifted_b, lifted_sum_b, gates_b = gates_of(
        sums[1 + experts], sums[2 + experts : 2 + 2 * experts], member_b
    )

    def by_slot(placed, values):
        return jnp.sum(jnp.where(placed, values[:, None, :], 0.0), axis=(0, 2))

    twice = lambda v: jnp.broadcast_to(v[None], (2, length))
    scalars = jnp.stack(
        [
            by_slot(placed_f, twice(r_f)),
            by_slot(placed_f, gates_f),
            by_slot(placed_b, twice(r_b)),
            by_slot(placed_b, gates_b),
        ]
    )
    scalars = exchanged(scalars.reshape(4, experts, capacity).transpose(1, 0, 2), "dp")
    scalars = scalars.transpose(1, 0, 2).reshape(4, slots)
    row_r = jnp.concatenate([scalars[0], scalars[2]])[:, None]
    row_gate = jnp.concatenate([scalars[1], scalars[3]])[:, None]

    at = lax.axis_index("expert")
    part = jax.ShapeDtypeStruct((experts // 2, 2 * capacity, width), BF16)
    *partial, gate_part, along_part, rows_gain = pl.pallas_call(
        functools.partial(expert_kernel, pieces),
        out_shape=(
            *[part] * (2 * pieces),
            jax.ShapeDtypeStruct((slots, 1), F32),
            jax.ShapeDtypeStruct((slots, 1), F32),
            jax.ShapeDtypeStruct((pieces, width), F32),
        ),
        in_specs=[pl.BlockSpec(memory_space=pltpu.SMEM)] + [vmem] * (4 + 2 * pieces),
        out_specs=(vmem,) * (2 * pieces + 3),
        scratch_shapes=[pltpu.VMEM((2 * slots, 2 * hidden), F32)],
    )(at[None].astype(jnp.int32), gate_up, down_w, row_r, row_gate, *whole)
    summed = jnp.concatenate(ring_scatter(partial, "expert"), axis=0)

    parts = jnp.concatenate([gate_part[:, 0], along_part[:, 0]])
    parts = jnp.stack([jnp.broadcast_to(parts, (pieces, 2 * slots)), jnp.roll(rows_gain, at, axis=0)], 1)
    parts = exchanged(parts, "expert")
    parts = jnp.sum(parts, axis=0)
    rows_gain = parts[1]
    parts = parts[0].reshape(2, experts, capacity).transpose(1, 0, 2)
    parts = exchanged(parts, "dp")
    parts = parts.transpose(1, 0, 2).reshape(2, slots)

    def by_token(values):
        return jnp.sum(jnp.where(placed_b, values[None, :, None], 0.0), axis=1)

    back_gate = by_token(parts[0].astype(BF16).astype(F32))
    along = by_token(parts[1])
    mixed = jnp.sum(back_gate * lifted_b, axis=0, keepdims=True) / lifted_sum_b
    chosen_cot = ROUTE_SCALE * (back_gate - mixed) / lifted_sum_b * lifted_b * (1.0 - lifted_b)
    logit_cot = jnp.sum(member_b * chosen_cot[:, None, :], axis=0)
    inner_r = jnp.sum(gates_b * along + chosen_cot * chosen_b, axis=0)
    router_part = lax.dot_general(
        logit_cot,
        router.astype(F32),
        (((0,), (1,)), ((), ())),
        precision=lax.Precision.HIGHEST,
        preferred_element_type=F32,
    )
    own_gain = jnp.sum(router_part * stashed32 * r_b[:, None], axis=0)
    own_gain = own_gain + rows_gain / gain
    gain_total = exchanged(jnp.broadcast_to(own_gain, (experts, 1, width)), "dp")
    gain_total = jnp.sum(gain_total, axis=(0, 1))
    base = (
        incoming.astype(F32)
        + (r_b[:, None] * router_part) * gain
        - stashed32 * (r_b * r_b * inner_r / D)[:, None]
    )

    back = exchanged(summed, "dp")

    def gathered(spread, rows):
        return lax.dot_general(
            spread,
            rows.reshape(slots, width),
            (((0,), (0,)), ((), ())),
            preferred_element_type=F32,
        )

    produced = (tokens32 + gathered(spread_f, back[:, :capacity])).astype(BF16)
    passed_forward = shifted(produced, "pipe", 1)
    moe_cot = gathered(spread_b, back[:, capacity : 2 * capacity])
    cotangent = (base + (r_b[:, None] * moe_cot) * gain).astype(BF16)
    passed_backward = shifted(cotangent, "pipe", -1)
    return (
        produced[None],
        cotangent[None],
        passed_forward[None],
        passed_backward[None],
        gain_total[None],
    )


def solution(mesh):
    placed = (
        P("pipe", "dp", "expert"),
        P("pipe", "dp", "expert"),
        P("pipe", "dp", "expert"),
        P("pipe", "dp", None),
        P("pipe", "dp", None),
        P("pipe", "expert"),
        P("pipe", "expert", None),
        P("pipe", "dp", None, None, "expert"),
        P("pipe", "dp", "expert", None),
    )
    return jax.shard_map(
        local,
        mesh=mesh,
        in_specs=placed,
        out_specs=(
            P("pipe", "dp", "expert"),
            P("pipe", "dp", "expert"),
            P("pipe", "dp", "expert"),
            P("pipe", "dp", "expert"),
            P("pipe", "expert"),
        ),
        check_vma=False,
    )
```

```python
import jax
import jax.numpy as jnp
from jax import lax
from jax.experimental import pallas as pl
from jax.experimental.pallas import tpu as pltpu
from jax.sharding import PartitionSpec as P

D = 4096
ROUTE_SCALE = 2.827
EPSILON = 1e-05
F32 = jnp.float32
BF16 = jnp.bfloat16


def summed_over(values, axis):
    copies = jnp.broadcast_to(values, (lax.axis_size(axis), *values.shape))
    return jnp.sum(lax.all_to_all(copies, axis, split_axis=0, concat_axis=0, tiled=True), axis=0)


def exchanged(blocks, axis):
    return lax.all_to_all(blocks, axis, split_axis=0, concat_axis=0, tiled=True)


def shifted(block, axis, distance):
    devices = range(lax.axis_size(axis))
    route = [(i - distance, i) for i in devices if i - distance in devices]
    return lax.ppermute(block, axis, route)


def rotated(block, axis, distance):
    size = lax.axis_size(axis)
    return lax.ppermute(block, axis, [(i, (i + distance) % size) for i in range(size)])


def slots_of(routes, experts, capacity):
    length = routes.shape[0]
    names = routes.T
    member = (names[:, None, :] == jnp.arange(experts, dtype=jnp.int32)[None, :, None]).astype(F32)
    token = jnp.arange(length, dtype=jnp.int32)
    earlier = (token[:, None] < token[None, :]).astype(BF16)
    before = jnp.dot(
        jnp.sum(member, axis=0).astype(BF16), earlier, preferred_element_type=F32
    )
    position = jnp.sum(member * before[None], axis=1).astype(jnp.int32)
    slot = names * capacity + position
    every = jnp.arange(experts * capacity, dtype=jnp.int32)
    placed = slot[:, None, :] == every[None, :, None]
    return slot, placed, member


def gates_of(squares, raw_logits, member):
    scaling = lax.rsqrt(squares / D + EPSILON)
    chosen = jnp.sum(member * raw_logits[None], axis=1) * scaling[None]
    lifted = jax.nn.sigmoid(chosen)
    lifted_sum = jnp.sum(lifted, axis=0, keepdims=True)
    return scaling, chosen, lifted, lifted_sum, ROUTE_SCALE * lifted / lifted_sum


def dispatch_kernel(routes_f, routes_b, gain, tokens, stashed, incoming, sent):
    experts, _, width = sent.shape
    length = tokens.shape[0]
    capacity = sent.shape[1] // 3
    shape = (2 * experts, length)
    row = lax.broadcasted_iota(jnp.int32, shape, 0)
    forward = row < experts
    expert = jnp.where(forward, row, row - experts)

    def named(k):
        return (
            jnp.where(
                forward,
                jnp.broadcast_to(routes_f[k : k + 1, :], shape),
                jnp.broadcast_to(routes_b[k : k + 1, :], shape),
            )
            == expert
        )

    member = named(0) | named(1)
    square = (length, length)
    earlier = jnp.where(
        lax.broadcasted_iota(jnp.int32, square, 0) < lax.broadcasted_iota(jnp.int32, square, 1),
        1.0,
        0.0,
    ).astype(BF16)
    before = jnp.dot(
        jnp.where(member, 1.0, 0.0).astype(BF16), earlier, preferred_element_type=F32
    )
    place = jnp.where(member, before.astype(jnp.int32), -1)
    slot = lax.broadcasted_iota(jnp.int32, (capacity, length), 0)

    def spread(first):
        return jnp.concatenate(
            [
                jnp.where(slot == place[e : e + 1, :], 1.0, 0.0).astype(BF16)
                for e in range(first, first + experts)
            ],
            axis=0,
        )

    spread_f, spread_b = spread(0), spread(experts)
    scaled_f = (tokens[...].astype(F32) * gain[...]).astype(BF16)
    scaled_b = (stashed[...].astype(F32) * gain[...]).astype(BF16)
    for k, (moved, rows) in enumerate(
        ((spread_f, scaled_f), (spread_b, scaled_b), (spread_b, incoming[...]))
    ):
        routed = jnp.dot(moved, rows, preferred_element_type=F32).astype(BF16)
        for e in range(experts):
            sent[e, k * capacity : (k + 1) * capacity, :] = routed[
                e * capacity : (e + 1) * capacity
            ]


def expert_kernel(
    whole,
    gate_up_hbm,
    down_w,
    row_r,
    row_gate,
    partial,
    gate_part,
    along_part,
    gain_part,
    rows,
    outs,
    sums,
    gate_up,
    took,
    loaded,
    left,
):
    pieces, experts, _, width = whole.shape
    capacity = whole.shape[2] // 3
    slots = experts * capacity
    hidden = down_w.shape[0]

    def fetch(z, k):
        return pltpu.make_async_copy(
            whole.at[z, :, pl.ds(k * capacity, capacity), :], rows.at[z, k], took.at[z, k]
        )

    def load(z):
        part = pl.ds(z * width, width)
        return pltpu.make_async_copy(gate_up_hbm.at[part, :], gate_up.at[part, :], loaded.at[z])

    def put(z, k):
        return pltpu.make_async_copy(
            outs.at[z, k], partial.at[z, :, pl.ds(k * capacity, capacity), :], left.at[z, k]
        )

    for z in range(pieces):
        load(z).start()
        for k in range(3):
            fetch(z, k).start()
    weighted = None
    for z in range(pieces):
        part = slice(z * width, (z + 1) * width)
        load(z).wait()
        for k in range(3):
            fetch(z, k).wait()
        values = rows[z, 0:2].reshape(2 * slots, width)
        product = jnp.dot(values, gate_up[part, :], preferred_element_type=F32)
        incoming = rows[z, 2].reshape(slots, width)
        product_w = lax.dot_general(
            incoming, down_w[:, part], (((1,), (1,)), ((), ())), preferred_element_type=F32
        )
        if z == 0:
            sums[...] = product
            weighted = product_w
        else:
            sums[...] += product
            weighted += product_w
    first = sums[:, :hidden] * row_r[...]
    second = sums[:, hidden:] * row_r[...]
    lifted = jax.nn.sigmoid(first)
    activated = first * lifted
    inner = (activated * second).astype(BF16)
    inner_f = inner[:slots]
    first, second, lifted, activated = first[slots:], second[slots:], lifted[slots:], activated[slots:]
    gate_part[...] = jnp.sum(inner[slots:].astype(F32) * weighted, axis=1, keepdims=True)
    grad_first = (weighted * second * lifted * (1.0 + first * (1.0 - lifted))).astype(BF16)
    grad_second = (weighted * activated).astype(BF16)
    along_part[...] = jnp.sum(
        grad_first.astype(F32) * first + grad_second.astype(F32) * second, axis=1, keepdims=True
    )
    grads = jnp.concatenate([grad_first, grad_second], axis=1)
    gate_f, gate_b, r_b = row_gate[:slots], row_gate[slots:], row_r[slots:]
    for z in range(pieces):
        part = slice(z * width, (z + 1) * width)
        out_f = jnp.dot(inner_f, down_w[:, part], preferred_element_type=F32) * gate_f
        outs[z, 0] = out_f.astype(BF16).reshape(experts, capacity, width)
        put(z, 0).start()
        out_b = (
            lax.dot_general(
                grads, gate_up[part, :], (((1,), (1,)), ((), ())), preferred_element_type=F32
            )
            * gate_b
        )
        outs[z, 1] = out_b.astype(BF16).reshape(experts, capacity, width)
        put(z, 1).start()
        stashed = rows[z, 1].reshape(slots, width).astype(F32)
        gain_part[z : z + 1, :] = jnp.sum(out_b * r_b * stashed, axis=0, keepdims=True)
    for z in range(pieces):
        for k in range(2):
            put(z, k).wait()


def local(
    entering,
    pending,
    stashed_in,
    forward_routes,
    backward_routes,
    norm_gains,
    w_router,
    w_gateup,
    w_down,
):
    gain = norm_gains[0]
    router = w_router[0]
    gate_up = w_gateup[0, 0].reshape(D, -1)
    down_w = w_down[0, 0]
    hidden = down_w.shape[0]
    tokens, stashed, incoming = entering[0], stashed_in[0], pending[0]
    length, width = tokens.shape
    experts = router.shape[1]
    capacity = length * forward_routes.shape[2] // experts

    slots = experts * capacity
    pieces = lax.axis_size("expert")
    vmem = pl.BlockSpec(memory_space=pltpu.VMEM)
    hbm = pl.BlockSpec(memory_space=pltpu.HBM)
    sent = pl.pallas_call(
        dispatch_kernel,
        out_shape=jax.ShapeDtypeStruct((experts, 3 * capacity, width), BF16),
        in_specs=[vmem] * 6,
        out_specs=vmem,
    )(
        forward_routes[0].T,
        backward_routes[0].T,
        gain[None],
        tokens,
        stashed,
        incoming,
    )
    arrived = exchanged(sent, "dp")
    whole = lax.all_gather(arrived.reshape(3 * slots, width), "expert", axis=0, tiled=True)

    (tokens, stashed, incoming, gain, routes_f, routes_b), _ = lax.optimization_barrier(
        ((tokens, stashed, incoming, gain, forward_routes[0], backward_routes[0]), arrived)
    )
    slot_f, placed_f, member_f = slots_of(routes_f, experts, capacity)
    slot_b, placed_b, member_b = slots_of(routes_b, experts, capacity)
    spread_f = (placed_f[0] | placed_f[1]).astype(BF16)
    spread_b = (placed_b[0] | placed_b[1]).astype(BF16)
    tokens32, stashed32 = tokens.astype(F32), stashed.astype(F32)
    scaled_f2 = (tokens32 * gain).astype(BF16)
    scaled_b2 = (stashed32 * gain).astype(BF16)

    def sums_of(values32, scaled):
        squares = jnp.sum(values32 * values32, axis=-1)[None]
        logits = lax.dot_general(
            router, scaled, (((0,), (1,)), ((), ())), preferred_element_type=F32
        )
        return [squares, logits]

    sums = jnp.concatenate(
        sums_of(tokens32, scaled_f2)
        + sums_of(stashed32, scaled_b2)
        + [jnp.zeros((16 - 2 * (experts + 1), length), F32)],
        axis=0,
    )
    sums = summed_over(sums, "expert")
    r_f, _, _, _, gates_f = gates_of(sums[0], sums[1 : 1 + experts], member_f)
    r_b, chosen_b, lifted_b, lifted_sum_b, gates_b = gates_of(
        sums[1 + experts], sums[2 + experts : 2 + 2 * experts], member_b
    )

    def by_slot(placed, values):
        return jnp.sum(jnp.where(placed, values[:, None, :], 0.0), axis=(0, 2))

    twice = lambda v: jnp.broadcast_to(v[None], (2, length))
    scalars = jnp.stack(
        [
            by_slot(placed_f, twice(r_f)),
            by_slot(placed_f, gates_f),
            by_slot(placed_b, twice(r_b)),
            by_slot(placed_b, gates_b),
        ]
    )
    scalars = exchanged(scalars.reshape(4, experts, capacity).transpose(1, 0, 2), "dp")
    scalars = scalars.transpose(1, 0, 2).reshape(4, slots)
    row_r = jnp.concatenate([scalars[0], scalars[2]])[:, None]
    row_gate = jnp.concatenate([scalars[1], scalars[3]])[:, None]

    partial, gate_part, along_part, rows_gain = pl.pallas_call(
        expert_kernel,
        out_shape=(
            jax.ShapeDtypeStruct((pieces, experts, 2 * capacity, width), BF16),
            jax.ShapeDtypeStruct((slots, 1), F32),
            jax.ShapeDtypeStruct((slots, 1), F32),
            jax.ShapeDtypeStruct((pieces, width), F32),
        ),
        in_specs=[hbm] * 2 + [vmem] * 3,
        out_specs=(hbm, vmem, vmem, vmem),
        scratch_shapes=[
            pltpu.VMEM((pieces, 3, experts, capacity, width), BF16),
            pltpu.VMEM((pieces, 2, experts, capacity, width), BF16),
            pltpu.VMEM((2 * slots, 2 * hidden), F32),
            pltpu.VMEM((D, 2 * hidden), BF16),
            pltpu.SemaphoreType.DMA((pieces, 3)),
            pltpu.SemaphoreType.DMA((pieces,)),
            pltpu.SemaphoreType.DMA((pieces, 2)),
        ],
    )(whole.reshape(pieces, experts, 3 * capacity, width), gate_up, down_w, row_r, row_gate)
    summed = lax.psum_scatter(
        partial.reshape(pieces * 2 * slots, width), "expert", scatter_dimension=0, tiled=True
    )
    summed = summed.reshape(experts, 2 * capacity, width)

    parts = jnp.concatenate([gate_part[:, 0], along_part[:, 0]])
    parts = jnp.stack([jnp.broadcast_to(parts, (pieces, 2 * slots)), rows_gain], 1)
    parts = exchanged(parts, "expert")
    parts = jnp.sum(parts, axis=0)
    rows_gain = parts[1]
    parts = parts[0].reshape(2, experts, capacity).transpose(1, 0, 2)
    parts = exchanged(parts, "dp")
    parts = parts.transpose(1, 0, 2).reshape(2, slots)

    def by_token(values):
        return jnp.sum(jnp.where(placed_b, values[None, :, None], 0.0), axis=1)

    back_gate = by_token(parts[0].astype(BF16).astype(F32))
    along = by_token(parts[1])
    mixed = jnp.sum(back_gate * lifted_b, axis=0, keepdims=True) / lifted_sum_b
    chosen_cot = ROUTE_SCALE * (back_gate - mixed) / lifted_sum_b * lifted_b * (1.0 - lifted_b)
    logit_cot = jnp.sum(member_b * chosen_cot[:, None, :], axis=0)
    inner_r = jnp.sum(gates_b * along + chosen_cot * chosen_b, axis=0)
    router_part = lax.dot_general(
        logit_cot,
        router.astype(F32),
        (((0,), (1,)), ((), ())),
        precision=lax.Precision.HIGHEST,
        preferred_element_type=F32,
    )
    own_gain = jnp.sum(router_part * stashed32 * r_b[:, None], axis=0)
    gain_total = summed_over((own_gain + rows_gain / gain)[None], "dp")[0]
    summed, gain_total = lax.optimization_barrier((summed, gain_total))
    base = (
        incoming.astype(F32)
        + (r_b[:, None] * router_part) * gain
        - stashed32 * (r_b * r_b * inner_r / D)[:, None]
    )

    back = exchanged(summed, "dp")
    def gathered(spread, rows):
        return lax.dot_general(
            spread,
            rows.reshape(slots, width),
            (((0,), (0,)), ((), ())),
            preferred_element_type=F32,
        )

    produced = (tokens32 + gathered(spread_f, back[:, :capacity])).astype(BF16)
    passed_forward = shifted(produced, "pipe", 1)
    moe_cot = gathered(spread_b, back[:, capacity : 2 * capacity])
    cotangent = (base + (r_b[:, None] * moe_cot) * gain).astype(BF16)
    passed_backward = shifted(cotangent, "pipe", -1)
    return (
        produced[None],
        cotangent[None],
        passed_forward[None],
        passed_backward[None],
        gain_total[None],
    )


def solution(mesh):
    placed = (
        P("pipe", "dp", "expert"),
        P("pipe", "dp", "expert"),
        P("pipe", "dp", "expert"),
        P("pipe", "dp", None),
        P("pipe", "dp", None),
        P("pipe", "expert"),
        P("pipe", "expert", None),
        P("pipe", "dp", None, None, "expert"),
        P("pipe", "dp", "expert", None),
    )
    return jax.shard_map(
        local,
        mesh=mesh,
        in_specs=placed,
        out_specs=(
            P("pipe", "dp", "expert"),
            P("pipe", "dp", "expert"),
            P("pipe", "dp", "expert"),
            P("pipe", "dp", "expert"),
            P("pipe", "expert"),
        ),
        check_vma=False,
    )
```

```python
import functools

import jax
import jax.numpy as jnp
from jax import lax
from jax.experimental import pallas as pl
from jax.experimental.pallas import tpu as pltpu
from jax.sharding import PartitionSpec as P

D = 4096
ROUTE_SCALE = 2.827
EPSILON = 1e-05
F32 = jnp.float32
BF16 = jnp.bfloat16


def summed_over(values, axis):
    copies = jnp.broadcast_to(values, (lax.axis_size(axis), *values.shape))
    return jnp.sum(lax.all_to_all(copies, axis, split_axis=0, concat_axis=0, tiled=True), axis=0)


def exchanged(blocks, axis):
    return lax.all_to_all(blocks, axis, split_axis=0, concat_axis=0, tiled=True)


def shifted(block, axis, distance):
    devices = range(lax.axis_size(axis))
    route = [(i - distance, i) for i in devices if i - distance in devices]
    return lax.ppermute(block, axis, route)


def rotated(block, axis, distance):
    size = lax.axis_size(axis)
    return lax.ppermute(block, axis, [(i, (i + distance) % size) for i in range(size)])


def ring_gather(block, axis):
    size = lax.axis_size(axis)
    middle = size // 2
    found = [block] + [None] * (size - 1)
    for step in range(1, middle):
        found[size - step] = rotated(found[(size - step + 1) % size], axis, 1)
        found[step] = rotated(found[step - 1], axis, -1)
    found[middle] = rotated(found[middle + 1], axis, 1)
    return found


def slots_of(routes, experts, capacity):
    length = routes.shape[0]
    names = routes.T
    member = (names[:, None, :] == jnp.arange(experts, dtype=jnp.int32)[None, :, None]).astype(F32)
    token = jnp.arange(length, dtype=jnp.int32)
    earlier = (token[:, None] < token[None, :]).astype(BF16)
    before = jnp.dot(
        jnp.sum(member, axis=0).astype(BF16), earlier, preferred_element_type=F32
    )
    position = jnp.sum(member * before[None], axis=1).astype(jnp.int32)
    slot = names * capacity + position
    every = jnp.arange(experts * capacity, dtype=jnp.int32)
    placed = slot[:, None, :] == every[None, :, None]
    return slot, placed, member


def gates_of(squares, raw_logits, member):
    scaling = lax.rsqrt(squares / D + EPSILON)
    chosen = jnp.sum(member * raw_logits[None], axis=1) * scaling[None]
    lifted = jax.nn.sigmoid(chosen)
    lifted_sum = jnp.sum(lifted, axis=0, keepdims=True)
    return scaling, chosen, lifted, lifted_sum, ROUTE_SCALE * lifted / lifted_sum


def dispatch_kernel(routes_f, routes_b, gain, tokens, stashed, incoming, sent):
    experts, _, width = sent.shape
    length = tokens.shape[0]
    capacity = sent.shape[1] // 3
    shape = (2 * experts, length)
    row = lax.broadcasted_iota(jnp.int32, shape, 0)
    forward = row < experts
    expert = jnp.where(forward, row, row - experts)

    def named(k):
        return (
            jnp.where(
                forward,
                jnp.broadcast_to(routes_f[k : k + 1, :], shape),
                jnp.broadcast_to(routes_b[k : k + 1, :], shape),
            )
            == expert
        )

    member = named(0) | named(1)
    square = (length, length)
    earlier = jnp.where(
        lax.broadcasted_iota(jnp.int32, square, 0) < lax.broadcasted_iota(jnp.int32, square, 1),
        1.0,
        0.0,
    ).astype(BF16)
    before = jnp.dot(
        jnp.where(member, 1.0, 0.0).astype(BF16), earlier, preferred_element_type=F32
    )
    place = jnp.where(member, before.astype(jnp.int32), -1)
    slot = lax.broadcasted_iota(jnp.int32, (capacity, length), 0)

    def spread(first):
        return jnp.concatenate(
            [
                jnp.where(slot == place[e : e + 1, :], 1.0, 0.0).astype(BF16)
                for e in range(first, first + experts)
            ],
            axis=0,
        )

    spread_f, spread_b = spread(0), spread(experts)
    scaled_f = (tokens[...].astype(F32) * gain[...]).astype(BF16)
    scaled_b = (stashed[...].astype(F32) * gain[...]).astype(BF16)
    for k, (moved, rows) in enumerate(
        ((spread_f, scaled_f), (spread_b, scaled_b), (spread_b, incoming[...]))
    ):
        routed = jnp.dot(moved, rows, preferred_element_type=F32).astype(BF16)
        for e in range(experts):
            sent[e, k * capacity : (k + 1) * capacity, :] = routed[
                e * capacity : (e + 1) * capacity
            ]


def expert_kernel(
    pieces,
    at,
    whole,
    gate_up_hbm,
    down_w,
    row_r,
    row_gate,
    *refs,
):
    ringed, refs = refs[:pieces], refs[pieces:]
    partial, gate_part, along_part, gain_part, rows, outs, sums, gate_up, took, came, loaded, left = refs
    experts, capacity, width = rows.shape[2:]
    slots = experts * capacity
    hidden = down_w.shape[0]

    def fetch(z, k, e):
        return pltpu.make_async_copy(
            whole.at[z, pl.ds((3 * e + k) * capacity, capacity), :],
            rows.at[z, k, e],
            took.at[z, k, e],
        )

    fetched = [(k, e) for k in range(3) for e in range(experts) if k == 0 or e < experts - 1]

    def place(j, k):
        return pltpu.make_async_copy(
            ringed[j].at[pl.ds((k - 1) * capacity, capacity), :],
            rows.at[(at[0] + j) % pieces, k, experts - 1],
            came.at[j, k - 1],
        )

    def load(z):
        part = pl.ds(z * width, width)
        return pltpu.make_async_copy(gate_up_hbm.at[part, :], gate_up.at[part, :], loaded.at[z])

    def put(z, k):
        return pltpu.make_async_copy(
            outs.at[z, k], partial.at[z, :, pl.ds(k * capacity, capacity), :], left.at[z, k]
        )

    for z in range(pieces):
        load(z).start()
        for k, e in fetched:
            fetch(z, k, e).start()
        for k in range(1, 3):
            place(z, k).start()
    for j in range(pieces):
        for k in range(1, 3):
            place(j, k).wait()
    weighted = None
    for z in range(pieces):
        part = slice(z * width, (z + 1) * width)
        load(z).wait()
        for k, e in fetched:
            fetch(z, k, e).wait()
        values = rows[z, 0:2].reshape(2 * slots, width)
        product = jnp.dot(values, gate_up[part, :], preferred_element_type=F32)
        incoming = rows[z, 2].reshape(slots, width)
        product_w = lax.dot_general(
            incoming, down_w[:, part], (((1,), (1,)), ((), ())), preferred_element_type=F32
        )
        if z == 0:
            sums[...] = product
            weighted = product_w
        else:
            sums[...] += product
            weighted += product_w
    first = sums[:, :hidden] * row_r[...]
    second = sums[:, hidden:] * row_r[...]
    lifted = jax.nn.sigmoid(first)
    activated = first * lifted
    inner = (activated * second).astype(BF16)
    inner_f = inner[:slots]
    first, second, lifted, activated = first[slots:], second[slots:], lifted[slots:], activated[slots:]
    gate_part[...] = jnp.sum(inner[slots:].astype(F32) * weighted, axis=1, keepdims=True)
    grad_first = (weighted * second * lifted * (1.0 + first * (1.0 - lifted))).astype(BF16)
    grad_second = (weighted * activated).astype(BF16)
    along_part[...] = jnp.sum(
        grad_first.astype(F32) * first + grad_second.astype(F32) * second, axis=1, keepdims=True
    )
    grads = jnp.concatenate([grad_first, grad_second], axis=1)
    gate_f, gate_b, r_b = row_gate[:slots], row_gate[slots:], row_r[slots:]
    for z in range(pieces):
        part = slice(z * width, (z + 1) * width)
        out_f = jnp.dot(inner_f, down_w[:, part], preferred_element_type=F32) * gate_f
        outs[z, 0] = out_f.astype(BF16).reshape(experts, capacity, width)
        put(z, 0).start()
        out_b = (
            lax.dot_general(
                grads, gate_up[part, :], (((1,), (1,)), ((), ())), preferred_element_type=F32
            )
            * gate_b
        )
        outs[z, 1] = out_b.astype(BF16).reshape(experts, capacity, width)
        put(z, 1).start()
        stashed = rows[z, 1].reshape(slots, width).astype(F32)
        gain_part[z : z + 1, :] = jnp.sum(out_b * r_b * stashed, axis=0, keepdims=True)
    for z in range(pieces):
        for k in range(2):
            put(z, k).wait()


def local(
    entering,
    pending,
    stashed_in,
    forward_routes,
    backward_routes,
    norm_gains,
    w_router,
    w_gateup,
    w_down,
):
    gain = norm_gains[0]
    router = w_router[0]
    gate_up = w_gateup[0, 0].reshape(D, -1)
    down_w = w_down[0, 0]
    hidden = down_w.shape[0]
    tokens, stashed, incoming = entering[0], stashed_in[0], pending[0]
    length, width = tokens.shape
    experts = router.shape[1]
    capacity = length * forward_routes.shape[2] // experts

    slots = experts * capacity
    pieces = lax.axis_size("expert")
    vmem = pl.BlockSpec(memory_space=pltpu.VMEM)
    hbm = pl.BlockSpec(memory_space=pltpu.HBM)
    sent = pl.pallas_call(
        dispatch_kernel,
        out_shape=jax.ShapeDtypeStruct((experts, 3 * capacity, width), BF16),
        in_specs=[vmem] * 6,
        out_specs=vmem,
    )(
        forward_routes[0].T,
        backward_routes[0].T,
        gain[None],
        tokens,
        stashed,
        incoming,
    )
    arrived = exchanged(sent, "dp")
    arrived_rows = arrived.reshape(3 * slots, width)
    native = 3 * slots - 2 * capacity
    whole = lax.all_gather(arrived_rows[:native], "expert", axis=0, tiled=True)
    ringed = ring_gather(arrived_rows[native:], "expert")

    (tokens, stashed, incoming, gain, routes_f, routes_b), _ = lax.optimization_barrier(
        ((tokens, stashed, incoming, gain, forward_routes[0], backward_routes[0]), arrived)
    )
    slot_f, placed_f, member_f = slots_of(routes_f, experts, capacity)
    slot_b, placed_b, member_b = slots_of(routes_b, experts, capacity)
    spread_f = (placed_f[0] | placed_f[1]).astype(BF16)
    spread_b = (placed_b[0] | placed_b[1]).astype(BF16)
    tokens32, stashed32 = tokens.astype(F32), stashed.astype(F32)
    scaled_f2 = (tokens32 * gain).astype(BF16)
    scaled_b2 = (stashed32 * gain).astype(BF16)

    def sums_of(values32, scaled):
        squares = jnp.sum(values32 * values32, axis=-1)[None]
        logits = lax.dot_general(
            router, scaled, (((0,), (1,)), ((), ())), preferred_element_type=F32
        )
        return [squares, logits]

    sums = jnp.concatenate(
        sums_of(tokens32, scaled_f2)
        + sums_of(stashed32, scaled_b2)
        + [jnp.zeros((16 - 2 * (experts + 1), length), F32)],
        axis=0,
    )
    sums = summed_over(sums, "expert")
    r_f, _, _, _, gates_f = gates_of(sums[0], sums[1 : 1 + experts], member_f)
    r_b, chosen_b, lifted_b, lifted_sum_b, gates_b = gates_of(
        sums[1 + experts], sums[2 + experts : 2 + 2 * experts], member_b
    )

    def by_slot(placed, values):
        return jnp.sum(jnp.where(placed, values[:, None, :], 0.0), axis=(0, 2))

    twice = lambda v: jnp.broadcast_to(v[None], (2, length))
    scalars = jnp.stack(
        [
            by_slot(placed_f, twice(r_f)),
            by_slot(placed_f, gates_f),
            by_slot(placed_b, twice(r_b)),
            by_slot(placed_b, gates_b),
        ]
    )
    scalars = exchanged(scalars.reshape(4, experts, capacity).transpose(1, 0, 2), "dp")
    scalars = scalars.transpose(1, 0, 2).reshape(4, slots)
    row_r = jnp.concatenate([scalars[0], scalars[2]])[:, None]
    row_gate = jnp.concatenate([scalars[1], scalars[3]])[:, None]

    partial, gate_part, along_part, rows_gain = pl.pallas_call(
        functools.partial(expert_kernel, pieces),
        out_shape=(
            jax.ShapeDtypeStruct((pieces, experts, 2 * capacity, width), BF16),
            jax.ShapeDtypeStruct((slots, 1), F32),
            jax.ShapeDtypeStruct((slots, 1), F32),
            jax.ShapeDtypeStruct((pieces, width), F32),
        ),
        in_specs=[pl.BlockSpec(memory_space=pltpu.SMEM)] + [hbm] * 2 + [vmem] * 3 + [hbm] * pieces,
        out_specs=(hbm, vmem, vmem, vmem),
        scratch_shapes=[
            pltpu.VMEM((pieces, 3, experts, capacity, width), BF16),
            pltpu.VMEM((pieces, 2, experts, capacity, width), BF16),
            pltpu.VMEM((2 * slots, 2 * hidden), F32),
            pltpu.VMEM((D, 2 * hidden), BF16),
            pltpu.SemaphoreType.DMA((pieces, 3, experts)),
            pltpu.SemaphoreType.DMA((pieces, 2)),
            pltpu.SemaphoreType.DMA((pieces,)),
            pltpu.SemaphoreType.DMA((pieces, 2)),
        ],
    )(
        lax.axis_index("expert")[None].astype(jnp.int32),
        whole.reshape(pieces, native, width),
        gate_up,
        down_w,
        row_r,
        row_gate,
        *ringed,
    )
    summed = lax.psum_scatter(
        partial.reshape(pieces * 2 * slots, width), "expert", scatter_dimension=0, tiled=True
    )
    summed = summed.reshape(experts, 2 * capacity, width)

    parts = jnp.concatenate([gate_part[:, 0], along_part[:, 0]])
    parts = jnp.stack([jnp.broadcast_to(parts, (pieces, 2 * slots)), rows_gain], 1)
    parts = exchanged(parts, "expert")
    parts = jnp.sum(parts, axis=0)
    rows_gain = parts[1]
    parts = parts[0].reshape(2, experts, capacity).transpose(1, 0, 2)
    parts = exchanged(parts, "dp")
    parts = parts.transpose(1, 0, 2).reshape(2, slots)

    def by_token(values):
        return jnp.sum(jnp.where(placed_b, values[None, :, None], 0.0), axis=1)

    back_gate = by_token(parts[0].astype(BF16).astype(F32))
    along = by_token(parts[1])
    mixed = jnp.sum(back_gate * lifted_b, axis=0, keepdims=True) / lifted_sum_b
    chosen_cot = ROUTE_SCALE * (back_gate - mixed) / lifted_sum_b * lifted_b * (1.0 - lifted_b)
    logit_cot = jnp.sum(member_b * chosen_cot[:, None, :], axis=0)
    inner_r = jnp.sum(gates_b * along + chosen_cot * chosen_b, axis=0)
    router_part = lax.dot_general(
        logit_cot,
        router.astype(F32),
        (((0,), (1,)), ((), ())),
        precision=lax.Precision.HIGHEST,
        preferred_element_type=F32,
    )
    own_gain = jnp.sum(router_part * stashed32 * r_b[:, None], axis=0)
    gain_total = summed_over((own_gain + rows_gain / gain)[None], "dp")[0]
    summed, gain_total = lax.optimization_barrier((summed, gain_total))
    base = (
        incoming.astype(F32)
        + (r_b[:, None] * router_part) * gain
        - stashed32 * (r_b * r_b * inner_r / D)[:, None]
    )

    back = exchanged(summed, "dp")
    def gathered(spread, rows):
        return lax.dot_general(
            spread,
            rows.reshape(slots, width),
            (((0,), (0,)), ((), ())),
            preferred_element_type=F32,
        )

    produced = (tokens32 + gathered(spread_f, back[:, :capacity])).astype(BF16)
    passed_forward = shifted(produced, "pipe", 1)
    moe_cot = gathered(spread_b, back[:, capacity : 2 * capacity])
    cotangent = (base + (r_b[:, None] * moe_cot) * gain).astype(BF16)
    passed_backward = shifted(cotangent, "pipe", -1)
    return (
        produced[None],
        cotangent[None],
        passed_forward[None],
        passed_backward[None],
        gain_total[None],
    )


def solution(mesh):
    placed = (
        P("pipe", "dp", "expert"),
        P("pipe", "dp", "expert"),
        P("pipe", "dp", "expert"),
        P("pipe", "dp", None),
        P("pipe", "dp", None),
        P("pipe", "expert"),
        P("pipe", "expert", None),
        P("pipe", "dp", None, None, "expert"),
        P("pipe", "dp", "expert", None),
    )
    return jax.shard_map(
        local,
        mesh=mesh,
        in_specs=placed,
        out_specs=(
            P("pipe", "dp", "expert"),
            P("pipe", "dp", "expert"),
            P("pipe", "dp", "expert"),
            P("pipe", "dp", "expert"),
            P("pipe", "expert"),
        ),
        check_vma=False,
    )
```

```python
import jax
import jax.numpy as jnp
from jax import lax
from jax.experimental import pallas as pl
from jax.experimental.pallas import tpu as pltpu
from jax.sharding import PartitionSpec as P

D = 4096
ROUTE_SCALE = 2.827
EPSILON = 1e-05
F32 = jnp.float32
BF16 = jnp.bfloat16


def summed_over(values, axis):
    copies = jnp.broadcast_to(values, (lax.axis_size(axis), *values.shape))
    return jnp.sum(lax.all_to_all(copies, axis, split_axis=0, concat_axis=0, tiled=True), axis=0)


def exchanged(blocks, axis):
    return lax.all_to_all(blocks, axis, split_axis=0, concat_axis=0, tiled=True)


def shifted(block, axis, distance):
    devices = range(lax.axis_size(axis))
    route = [(i - distance, i) for i in devices if i - distance in devices]
    return lax.ppermute(block, axis, route)


def rotated(block, axis, distance):
    size = lax.axis_size(axis)
    return lax.ppermute(block, axis, [(i, (i + distance) % size) for i in range(size)])


def slots_of(routes, experts, capacity):
    length = routes.shape[0]
    names = routes.T
    member = (names[:, None, :] == jnp.arange(experts, dtype=jnp.int32)[None, :, None]).astype(F32)
    token = jnp.arange(length, dtype=jnp.int32)
    earlier = (token[:, None] < token[None, :]).astype(BF16)
    before = jnp.dot(
        jnp.sum(member, axis=0).astype(BF16), earlier, preferred_element_type=F32
    )
    position = jnp.sum(member * before[None], axis=1).astype(jnp.int32)
    slot = names * capacity + position
    every = jnp.arange(experts * capacity, dtype=jnp.int32)
    placed = slot[:, None, :] == every[None, :, None]
    return slot, placed, member


def gates_of(squares, raw_logits, member):
    scaling = lax.rsqrt(squares / D + EPSILON)
    chosen = jnp.sum(member * raw_logits[None], axis=1) * scaling[None]
    lifted = jax.nn.sigmoid(chosen)
    lifted_sum = jnp.sum(lifted, axis=0, keepdims=True)
    return scaling, chosen, lifted, lifted_sum, ROUTE_SCALE * lifted / lifted_sum


def dispatch_kernel(routes_f, routes_b, gain, tokens, stashed, incoming, sent):
    experts, _, width = sent.shape
    length = tokens.shape[0]
    capacity = sent.shape[1] // 3
    shape = (2 * experts, length)
    row = lax.broadcasted_iota(jnp.int32, shape, 0)
    forward = row < experts
    expert = jnp.where(forward, row, row - experts)

    def named(k):
        return (
            jnp.where(
                forward,
                jnp.broadcast_to(routes_f[k : k + 1, :], shape),
                jnp.broadcast_to(routes_b[k : k + 1, :], shape),
            )
            == expert
        )

    member = named(0) | named(1)
    square = (length, length)
    earlier = jnp.where(
        lax.broadcasted_iota(jnp.int32, square, 0) < lax.broadcasted_iota(jnp.int32, square, 1),
        1.0,
        0.0,
    ).astype(BF16)
    before = jnp.dot(
        jnp.where(member, 1.0, 0.0).astype(BF16), earlier, preferred_element_type=F32
    )
    place = jnp.where(member, before.astype(jnp.int32), -1)
    slot = lax.broadcasted_iota(jnp.int32, (capacity, length), 0)

    def spread(first):
        return jnp.concatenate(
            [
                jnp.where(slot == place[e : e + 1, :], 1.0, 0.0).astype(BF16)
                for e in range(first, first + experts)
            ],
            axis=0,
        )

    spread_f, spread_b = spread(0), spread(experts)
    scaled_f = (tokens[...].astype(F32) * gain[...]).astype(BF16)
    scaled_b = (stashed[...].astype(F32) * gain[...]).astype(BF16)
    for k, (moved, rows) in enumerate(
        ((spread_f, scaled_f), (spread_b, scaled_b), (spread_b, incoming[...]))
    ):
        routed = jnp.dot(moved, rows, preferred_element_type=F32).astype(BF16)
        for e in range(experts):
            sent[e, k * capacity : (k + 1) * capacity, :] = routed[
                e * capacity : (e + 1) * capacity
            ]


def expert_kernel(
    whole,
    gate_up_hbm,
    down_w,
    row_r,
    row_gate,
    partial,
    gate_part,
    along_part,
    gain_part,
    rows,
    outs,
    sums,
    gate_up,
    took,
    loaded,
    left,
):
    pieces, experts, _, width = whole.shape
    capacity = whole.shape[2] // 3
    slots = experts * capacity
    hidden = down_w.shape[0]

    def fetch(z, k):
        return pltpu.make_async_copy(
            whole.at[z, :, pl.ds(k * capacity, capacity), :], rows.at[z, k], took.at[z, k]
        )

    def load(z):
        part = pl.ds(z * width, width)
        return pltpu.make_async_copy(gate_up_hbm.at[part, :], gate_up.at[part, :], loaded.at[z])

    def put(z, k):
        return pltpu.make_async_copy(
            outs.at[z, k], partial.at[z, :, pl.ds(k * capacity, capacity), :], left.at[z, k]
        )

    def begin(z):
        load(z).start()
        for k in range(3):
            fetch(z, k).start()

    ahead = pieces // 2
    for z in range(ahead):
        begin(z)
    weighted = None
    for z in range(pieces):
        part = slice(z * width, (z + 1) * width)
        load(z).wait()
        fetch(z, 0).wait()
        if z + ahead < pieces:
            begin(z + ahead)
        fetch(z, 1).wait()
        values = rows[z, 0:2].reshape(2 * slots, width)
        product = jnp.dot(values, gate_up[part, :], preferred_element_type=F32)
        fetch(z, 2).wait()
        incoming = rows[z, 2].reshape(slots, width)
        product_w = lax.dot_general(
            incoming, down_w[:, part], (((1,), (1,)), ((), ())), preferred_element_type=F32
        )
        if z == 0:
            sums[...] = product
            weighted = product_w
        else:
            sums[...] += product
            weighted += product_w
    first = sums[:, :hidden] * row_r[...]
    second = sums[:, hidden:] * row_r[...]
    lifted = jax.nn.sigmoid(first)
    activated = first * lifted
    inner = (activated * second).astype(BF16)
    inner_f = inner[:slots]
    first, second, lifted, activated = first[slots:], second[slots:], lifted[slots:], activated[slots:]
    gate_part[...] = jnp.sum(inner[slots:].astype(F32) * weighted, axis=1, keepdims=True)
    grad_first = (weighted * second * lifted * (1.0 + first * (1.0 - lifted))).astype(BF16)
    grad_second = (weighted * activated).astype(BF16)
    along_part[...] = jnp.sum(
        grad_first.astype(F32) * first + grad_second.astype(F32) * second, axis=1, keepdims=True
    )
    grads = jnp.concatenate([grad_first, grad_second], axis=1)
    gate_f, gate_b, r_b = row_gate[:slots], row_gate[slots:], row_r[slots:]
    for z in range(pieces):
        part = slice(z * width, (z + 1) * width)
        out_f = jnp.dot(inner_f, down_w[:, part], preferred_element_type=F32) * gate_f
        outs[z, 0] = out_f.astype(BF16).reshape(experts, capacity, width)
        put(z, 0).start()
        out_b = (
            lax.dot_general(
                grads, gate_up[part, :], (((1,), (1,)), ((), ())), preferred_element_type=F32
            )
            * gate_b
        )
        outs[z, 1] = out_b.astype(BF16).reshape(experts, capacity, width)
        put(z, 1).start()
        stashed = rows[z, 1].reshape(slots, width).astype(F32)
        gain_part[z : z + 1, :] = jnp.sum(out_b * r_b * stashed, axis=0, keepdims=True)
    for z in range(pieces):
        for k in range(2):
            put(z, k).wait()


def local(
    entering,
    pending,
    stashed_in,
    forward_routes,
    backward_routes,
    norm_gains,
    w_router,
    w_gateup,
    w_down,
):
    gain = norm_gains[0]
    router = w_router[0]
    gate_up = w_gateup[0, 0].reshape(D, -1)
    down_w = w_down[0, 0]
    hidden = down_w.shape[0]
    tokens, stashed, incoming = entering[0], stashed_in[0], pending[0]
    length, width = tokens.shape
    experts = router.shape[1]
    capacity = length * forward_routes.shape[2] // experts

    slots = experts * capacity
    pieces = lax.axis_size("expert")
    vmem = pl.BlockSpec(memory_space=pltpu.VMEM)
    hbm = pl.BlockSpec(memory_space=pltpu.HBM)
    sent = pl.pallas_call(
        dispatch_kernel,
        out_shape=jax.ShapeDtypeStruct((experts, 3 * capacity, width), BF16),
        in_specs=[vmem] * 6,
        out_specs=vmem,
    )(
        forward_routes[0].T,
        backward_routes[0].T,
        gain[None],
        tokens,
        stashed,
        incoming,
    )
    arrived = exchanged(sent, "dp")
    whole = lax.all_gather(arrived.reshape(3 * slots, width), "expert", axis=0, tiled=True)

    (tokens, stashed, incoming, gain, routes_f, routes_b), _ = lax.optimization_barrier(
        ((tokens, stashed, incoming, gain, forward_routes[0], backward_routes[0]), arrived)
    )
    slot_f, placed_f, member_f = slots_of(routes_f, experts, capacity)
    slot_b, placed_b, member_b = slots_of(routes_b, experts, capacity)
    spread_f = (placed_f[0] | placed_f[1]).astype(BF16)
    spread_b = (placed_b[0] | placed_b[1]).astype(BF16)
    tokens32, stashed32 = tokens.astype(F32), stashed.astype(F32)
    scaled_f2 = (tokens32 * gain).astype(BF16)
    scaled_b2 = (stashed32 * gain).astype(BF16)

    def sums_of(values32, scaled):
        squares = jnp.sum(values32 * values32, axis=-1)[None]
        logits = lax.dot_general(
            router, scaled, (((0,), (1,)), ((), ())), preferred_element_type=F32
        )
        return [squares, logits]

    sums = jnp.concatenate(
        sums_of(tokens32, scaled_f2)
        + sums_of(stashed32, scaled_b2)
        + [jnp.zeros((16 - 2 * (experts + 1), length), F32)],
        axis=0,
    )
    sums = summed_over(sums, "expert")
    r_f, _, _, _, gates_f = gates_of(sums[0], sums[1 : 1 + experts], member_f)
    r_b, chosen_b, lifted_b, lifted_sum_b, gates_b = gates_of(
        sums[1 + experts], sums[2 + experts : 2 + 2 * experts], member_b
    )

    def by_slot(placed, values):
        return jnp.sum(jnp.where(placed, values[:, None, :], 0.0), axis=(0, 2))

    twice = lambda v: jnp.broadcast_to(v[None], (2, length))
    scalars = jnp.stack(
        [
            by_slot(placed_f, twice(r_f)),
            by_slot(placed_f, gates_f),
            by_slot(placed_b, twice(r_b)),
            by_slot(placed_b, gates_b),
        ]
    )
    scalars = exchanged(scalars.reshape(4, experts, capacity).transpose(1, 0, 2), "dp")
    scalars = scalars.transpose(1, 0, 2).reshape(4, slots)
    row_r = jnp.concatenate([scalars[0], scalars[2]])[:, None]
    row_gate = jnp.concatenate([scalars[1], scalars[3]])[:, None]

    partial, gate_part, along_part, rows_gain = pl.pallas_call(
        expert_kernel,
        out_shape=(
            jax.ShapeDtypeStruct((pieces, experts, 2 * capacity, width), BF16),
            jax.ShapeDtypeStruct((slots, 1), F32),
            jax.ShapeDtypeStruct((slots, 1), F32),
            jax.ShapeDtypeStruct((pieces, width), F32),
        ),
        in_specs=[hbm] * 2 + [vmem] * 3,
        out_specs=(hbm, vmem, vmem, vmem),
        scratch_shapes=[
            pltpu.VMEM((pieces, 3, experts, capacity, width), BF16),
            pltpu.VMEM((pieces, 2, experts, capacity, width), BF16),
            pltpu.VMEM((2 * slots, 2 * hidden), F32),
            pltpu.VMEM((D, 2 * hidden), BF16),
            pltpu.SemaphoreType.DMA((pieces, 3)),
            pltpu.SemaphoreType.DMA((pieces,)),
            pltpu.SemaphoreType.DMA((pieces, 2)),
        ],
    )(whole.reshape(pieces, experts, 3 * capacity, width), gate_up, down_w, row_r, row_gate)
    summed = lax.psum_scatter(
        partial.reshape(pieces * 2 * slots, width), "expert", scatter_dimension=0, tiled=True
    )
    summed = summed.reshape(experts, 2 * capacity, width)

    parts = jnp.concatenate([gate_part[:, 0], along_part[:, 0]])
    parts = jnp.stack([jnp.broadcast_to(parts, (pieces, 2 * slots)), rows_gain], 1)
    parts = exchanged(parts, "expert")
    parts = jnp.sum(parts, axis=0)
    rows_gain = parts[1]
    parts = parts[0].reshape(2, experts, capacity).transpose(1, 0, 2)
    parts = exchanged(parts, "dp")
    parts = parts.transpose(1, 0, 2).reshape(2, slots)

    def by_token(values):
        return jnp.sum(jnp.where(placed_b, values[None, :, None], 0.0), axis=1)

    back_gate = by_token(parts[0].astype(BF16).astype(F32))
    along = by_token(parts[1])
    mixed = jnp.sum(back_gate * lifted_b, axis=0, keepdims=True) / lifted_sum_b
    chosen_cot = ROUTE_SCALE * (back_gate - mixed) / lifted_sum_b * lifted_b * (1.0 - lifted_b)
    logit_cot = jnp.sum(member_b * chosen_cot[:, None, :], axis=0)
    inner_r = jnp.sum(gates_b * along + chosen_cot * chosen_b, axis=0)
    router_part = lax.dot_general(
        logit_cot,
        router.astype(F32),
        (((0,), (1,)), ((), ())),
        precision=lax.Precision.HIGHEST,
        preferred_element_type=F32,
    )
    own_gain = jnp.sum(router_part * stashed32 * r_b[:, None], axis=0)
    gain_total = summed_over((own_gain + rows_gain / gain)[None], "dp")[0]
    summed, gain_total = lax.optimization_barrier((summed, gain_total))
    base = (
        incoming.astype(F32)
        + (r_b[:, None] * router_part) * gain
        - stashed32 * (r_b * r_b * inner_r / D)[:, None]
    )

    back = exchanged(summed, "dp")
    def gathered(spread, rows):
        return lax.dot_general(
            spread,
            rows.reshape(slots, width),
            (((0,), (0,)), ((), ())),
            preferred_element_type=F32,
        )

    produced = (tokens32 + gathered(spread_f, back[:, :capacity])).astype(BF16)
    passed_forward = shifted(produced, "pipe", 1)
    moe_cot = gathered(spread_b, back[:, capacity : 2 * capacity])
    cotangent = (base + (r_b[:, None] * moe_cot) * gain).astype(BF16)
    passed_backward = shifted(cotangent, "pipe", -1)
    return (
        produced[None],
        cotangent[None],
        passed_forward[None],
        passed_backward[None],
        gain_total[None],
    )


def solution(mesh):
    placed = (
        P("pipe", "dp", "expert"),
        P("pipe", "dp", "expert"),
        P("pipe", "dp", "expert"),
        P("pipe", "dp", None),
        P("pipe", "dp", None),
        P("pipe", "expert"),
        P("pipe", "expert", None),
        P("pipe", "dp", None, None, "expert"),
        P("pipe", "dp", "expert", None),
    )
    return jax.shard_map(
        local,
        mesh=mesh,
        in_specs=placed,
        out_specs=(
            P("pipe", "dp", "expert"),
            P("pipe", "dp", "expert"),
            P("pipe", "dp", "expert"),
            P("pipe", "dp", "expert"),
            P("pipe", "expert"),
        ),
        check_vma=False,
    )
```

```python
import jax
import jax.numpy as jnp
from jax import lax
from jax.experimental import pallas as pl
from jax.experimental.pallas import tpu as pltpu
from jax.sharding import PartitionSpec as P

D = 4096
ROUTE_SCALE = 2.827
EPSILON = 1e-05
F32 = jnp.float32
BF16 = jnp.bfloat16


def summed_over(values, axis):
    copies = jnp.broadcast_to(values, (lax.axis_size(axis), *values.shape))
    return jnp.sum(lax.all_to_all(copies, axis, split_axis=0, concat_axis=0, tiled=True), axis=0)


def exchanged(blocks, axis):
    return lax.all_to_all(blocks, axis, split_axis=0, concat_axis=0, tiled=True)


def shifted(block, axis, distance):
    devices = range(lax.axis_size(axis))
    route = [(i - distance, i) for i in devices if i - distance in devices]
    return lax.ppermute(block, axis, route)


def rotated(block, axis, distance):
    size = lax.axis_size(axis)
    return lax.ppermute(block, axis, [(i, (i + distance) % size) for i in range(size)])


def slots_of(routes, experts, capacity):
    length = routes.shape[0]
    names = routes.T
    member = (names[:, None, :] == jnp.arange(experts, dtype=jnp.int32)[None, :, None]).astype(F32)
    token = jnp.arange(length, dtype=jnp.int32)
    earlier = (token[:, None] < token[None, :]).astype(BF16)
    before = jnp.dot(
        jnp.sum(member, axis=0).astype(BF16), earlier, preferred_element_type=F32
    )
    position = jnp.sum(member * before[None], axis=1).astype(jnp.int32)
    slot = names * capacity + position
    every = jnp.arange(experts * capacity, dtype=jnp.int32)
    placed = slot[:, None, :] == every[None, :, None]
    return slot, placed, member


def gates_of(squares, raw_logits, member):
    scaling = lax.rsqrt(squares / D + EPSILON)
    chosen = jnp.sum(member * raw_logits[None], axis=1) * scaling[None]
    lifted = jax.nn.sigmoid(chosen)
    lifted_sum = jnp.sum(lifted, axis=0, keepdims=True)
    return scaling, chosen, lifted, lifted_sum, ROUTE_SCALE * lifted / lifted_sum


def dispatch_kernel(routes_f, routes_b, gain, tokens, stashed, incoming, sent):
    experts, _, width = sent.shape
    length = tokens.shape[0]
    capacity = sent.shape[1] // 3
    shape = (2 * experts, length)
    row = lax.broadcasted_iota(jnp.int32, shape, 0)
    forward = row < experts
    expert = jnp.where(forward, row, row - experts)

    def named(k):
        return (
            jnp.where(
                forward,
                jnp.broadcast_to(routes_f[k : k + 1, :], shape),
                jnp.broadcast_to(routes_b[k : k + 1, :], shape),
            )
            == expert
        )

    member = named(0) | named(1)
    square = (length, length)
    earlier = jnp.where(
        lax.broadcasted_iota(jnp.int32, square, 0) < lax.broadcasted_iota(jnp.int32, square, 1),
        1.0,
        0.0,
    ).astype(BF16)
    before = jnp.dot(
        jnp.where(member, 1.0, 0.0).astype(BF16), earlier, preferred_element_type=F32
    )
    place = jnp.where(member, before.astype(jnp.int32), -1)
    slot = lax.broadcasted_iota(jnp.int32, (capacity, length), 0)

    def spread(first):
        return jnp.concatenate(
            [
                jnp.where(slot == place[e : e + 1, :], 1.0, 0.0).astype(BF16)
                for e in range(first, first + experts)
            ],
            axis=0,
        )

    spread_f, spread_b = spread(0), spread(experts)
    scaled_f = (tokens[...].astype(F32) * gain[...]).astype(BF16)
    scaled_b = (stashed[...].astype(F32) * gain[...]).astype(BF16)
    for k, (moved, rows) in enumerate(
        ((spread_f, scaled_f), (spread_b, scaled_b), (spread_b, incoming[...]))
    ):
        routed = jnp.dot(moved, rows, preferred_element_type=F32).astype(BF16)
        for e in range(experts):
            sent[e, k * capacity : (k + 1) * capacity, :] = routed[
                e * capacity : (e + 1) * capacity
            ]


def expert_kernel(
    whole,
    gate_up_hbm,
    down_w,
    row_r,
    row_gate,
    partial,
    gate_part,
    along_part,
    gain_part,
    rows,
    outs,
    sums,
    gate_up,
    took,
    loaded,
    left,
):
    pieces, experts, _, width = whole.shape
    capacity = whole.shape[2] // 3
    slots = experts * capacity
    hidden = down_w.shape[0]

    def fetch(z):
        return pltpu.make_async_copy(whole.at[z], rows.at[z], took.at[z])

    def taken(z, k):
        return rows[z, :, k * capacity : (k + 1) * capacity, :].reshape(slots, width)

    def load(z):
        part = pl.ds(z * width, width)
        return pltpu.make_async_copy(gate_up_hbm.at[part, :], gate_up.at[part, :], loaded.at[z])

    def put(z):
        return pltpu.make_async_copy(outs.at[z], partial.at[z], left.at[z])

    for z in range(pieces):
        load(z).start()
        fetch(z).start()
    weighted = None
    for z in range(pieces):
        part = slice(z * width, (z + 1) * width)
        load(z).wait()
        fetch(z).wait()
        values = jnp.concatenate([taken(z, 0), taken(z, 1)], axis=0)
        product = jnp.dot(values, gate_up[part, :], preferred_element_type=F32)
        incoming = taken(z, 2)
        product_w = lax.dot_general(
            incoming, down_w[:, part], (((1,), (1,)), ((), ())), preferred_element_type=F32
        )
        if z == 0:
            sums[...] = product
            weighted = product_w
        else:
            sums[...] += product
            weighted += product_w
    first = sums[:, :hidden] * row_r[...]
    second = sums[:, hidden:] * row_r[...]
    lifted = jax.nn.sigmoid(first)
    activated = first * lifted
    inner = (activated * second).astype(BF16)
    inner_f = inner[:slots]
    first, second, lifted, activated = first[slots:], second[slots:], lifted[slots:], activated[slots:]
    gate_part[...] = jnp.sum(inner[slots:].astype(F32) * weighted, axis=1, keepdims=True)
    grad_first = (weighted * second * lifted * (1.0 + first * (1.0 - lifted))).astype(BF16)
    grad_second = (weighted * activated).astype(BF16)
    along_part[...] = jnp.sum(
        grad_first.astype(F32) * first + grad_second.astype(F32) * second, axis=1, keepdims=True
    )
    grads = jnp.concatenate([grad_first, grad_second], axis=1)
    gate_f, gate_b, r_b = row_gate[:slots], row_gate[slots:], row_r[slots:]
    for z in range(pieces):
        part = slice(z * width, (z + 1) * width)
        out_f = jnp.dot(inner_f, down_w[:, part], preferred_element_type=F32) * gate_f
        outs[z, :, :capacity, :] = out_f.astype(BF16).reshape(experts, capacity, width)
        out_b = (
            lax.dot_general(
                grads, gate_up[part, :], (((1,), (1,)), ((), ())), preferred_element_type=F32
            )
            * gate_b
        )
        outs[z, :, capacity:, :] = out_b.astype(BF16).reshape(experts, capacity, width)
        put(z).start()
        stashed = taken(z, 1).astype(F32)
        gain_part[z : z + 1, :] = jnp.sum(out_b * r_b * stashed, axis=0, keepdims=True)
    for z in range(pieces):
        put(z).wait()


def local(
    entering,
    pending,
    stashed_in,
    forward_routes,
    backward_routes,
    norm_gains,
    w_router,
    w_gateup,
    w_down,
):
    gain = norm_gains[0]
    router = w_router[0]
    gate_up = w_gateup[0, 0].reshape(D, -1)
    down_w = w_down[0, 0]
    hidden = down_w.shape[0]
    tokens, stashed, incoming = entering[0], stashed_in[0], pending[0]
    length, width = tokens.shape
    experts = router.shape[1]
    capacity = length * forward_routes.shape[2] // experts

    slots = experts * capacity
    pieces = lax.axis_size("expert")
    vmem = pl.BlockSpec(memory_space=pltpu.VMEM)
    hbm = pl.BlockSpec(memory_space=pltpu.HBM)
    sent = pl.pallas_call(
        dispatch_kernel,
        out_shape=jax.ShapeDtypeStruct((experts, 3 * capacity, width), BF16),
        in_specs=[vmem] * 6,
        out_specs=vmem,
    )(
        forward_routes[0].T,
        backward_routes[0].T,
        gain[None],
        tokens,
        stashed,
        incoming,
    )
    arrived = exchanged(sent, "dp")
    whole = lax.all_gather(arrived.reshape(3 * slots, width), "expert", axis=0, tiled=True)

    (tokens, stashed, incoming, gain, routes_f, routes_b), _ = lax.optimization_barrier(
        ((tokens, stashed, incoming, gain, forward_routes[0], backward_routes[0]), arrived)
    )
    slot_f, placed_f, member_f = slots_of(routes_f, experts, capacity)
    slot_b, placed_b, member_b = slots_of(routes_b, experts, capacity)
    spread_f = (placed_f[0] | placed_f[1]).astype(BF16)
    spread_b = (placed_b[0] | placed_b[1]).astype(BF16)
    tokens32, stashed32 = tokens.astype(F32), stashed.astype(F32)
    scaled_f2 = (tokens32 * gain).astype(BF16)
    scaled_b2 = (stashed32 * gain).astype(BF16)

    def sums_of(values32, scaled):
        squares = jnp.sum(values32 * values32, axis=-1)[None]
        logits = lax.dot_general(
            router, scaled, (((0,), (1,)), ((), ())), preferred_element_type=F32
        )
        return [squares, logits]

    sums = jnp.concatenate(
        sums_of(tokens32, scaled_f2)
        + sums_of(stashed32, scaled_b2)
        + [jnp.zeros((16 - 2 * (experts + 1), length), F32)],
        axis=0,
    )
    sums = summed_over(sums, "expert")
    r_f, _, _, _, gates_f = gates_of(sums[0], sums[1 : 1 + experts], member_f)
    r_b, chosen_b, lifted_b, lifted_sum_b, gates_b = gates_of(
        sums[1 + experts], sums[2 + experts : 2 + 2 * experts], member_b
    )

    def by_slot(placed, values):
        return jnp.sum(jnp.where(placed, values[:, None, :], 0.0), axis=(0, 2))

    twice = lambda v: jnp.broadcast_to(v[None], (2, length))
    scalars = jnp.stack(
        [
            by_slot(placed_f, twice(r_f)),
            by_slot(placed_f, gates_f),
            by_slot(placed_b, twice(r_b)),
            by_slot(placed_b, gates_b),
        ]
    )
    scalars = exchanged(scalars.reshape(4, experts, capacity).transpose(1, 0, 2), "dp")
    scalars = scalars.transpose(1, 0, 2).reshape(4, slots)
    row_r = jnp.concatenate([scalars[0], scalars[2]])[:, None]
    row_gate = jnp.concatenate([scalars[1], scalars[3]])[:, None]

    partial, gate_part, along_part, rows_gain = pl.pallas_call(
        expert_kernel,
        out_shape=(
            jax.ShapeDtypeStruct((pieces, experts, 2 * capacity, width), BF16),
            jax.ShapeDtypeStruct((slots, 1), F32),
            jax.ShapeDtypeStruct((slots, 1), F32),
            jax.ShapeDtypeStruct((pieces, width), F32),
        ),
        in_specs=[hbm] * 2 + [vmem] * 3,
        out_specs=(hbm, vmem, vmem, vmem),
        scratch_shapes=[
            pltpu.VMEM((pieces, experts, 3 * capacity, width), BF16),
            pltpu.VMEM((pieces, experts, 2 * capacity, width), BF16),
            pltpu.VMEM((2 * slots, 2 * hidden), F32),
            pltpu.VMEM((D, 2 * hidden), BF16),
            pltpu.SemaphoreType.DMA((pieces,)),
            pltpu.SemaphoreType.DMA((pieces,)),
            pltpu.SemaphoreType.DMA((pieces,)),
        ],
    )(whole.reshape(pieces, experts, 3 * capacity, width), gate_up, down_w, row_r, row_gate)
    summed = lax.psum_scatter(
        partial.reshape(pieces * 2 * slots, width), "expert", scatter_dimension=0, tiled=True
    )
    summed = summed.reshape(experts, 2 * capacity, width)

    parts = jnp.concatenate([gate_part[:, 0], along_part[:, 0]])
    parts = jnp.stack([jnp.broadcast_to(parts, (pieces, 2 * slots)), rows_gain], 1)
    parts = exchanged(parts, "expert")
    parts = jnp.sum(parts, axis=0)
    rows_gain = parts[1]
    parts = parts[0].reshape(2, experts, capacity).transpose(1, 0, 2)
    parts = exchanged(parts, "dp")
    parts = parts.transpose(1, 0, 2).reshape(2, slots)

    def by_token(values):
        return jnp.sum(jnp.where(placed_b, values[None, :, None], 0.0), axis=1)

    back_gate = by_token(parts[0].astype(BF16).astype(F32))
    along = by_token(parts[1])
    mixed = jnp.sum(back_gate * lifted_b, axis=0, keepdims=True) / lifted_sum_b
    chosen_cot = ROUTE_SCALE * (back_gate - mixed) / lifted_sum_b * lifted_b * (1.0 - lifted_b)
    logit_cot = jnp.sum(member_b * chosen_cot[:, None, :], axis=0)
    inner_r = jnp.sum(gates_b * along + chosen_cot * chosen_b, axis=0)
    router_part = lax.dot_general(
        logit_cot,
        router.astype(F32),
        (((0,), (1,)), ((), ())),
        precision=lax.Precision.HIGHEST,
        preferred_element_type=F32,
    )
    own_gain = jnp.sum(router_part * stashed32 * r_b[:, None], axis=0)
    gain_total = summed_over((own_gain + rows_gain / gain)[None], "dp")[0]
    summed, gain_total = lax.optimization_barrier((summed, gain_total))
    base = (
        incoming.astype(F32)
        + (r_b[:, None] * router_part) * gain
        - stashed32 * (r_b * r_b * inner_r / D)[:, None]
    )

    back = exchanged(summed, "dp")
    def gathered(spread, rows):
        return lax.dot_general(
            spread,
            rows.reshape(slots, width),
            (((0,), (0,)), ((), ())),
            preferred_element_type=F32,
        )

    produced = (tokens32 + gathered(spread_f, back[:, :capacity])).astype(BF16)
    passed_forward = shifted(produced, "pipe", 1)
    moe_cot = gathered(spread_b, back[:, capacity : 2 * capacity])
    cotangent = (base + (r_b[:, None] * moe_cot) * gain).astype(BF16)
    passed_backward = shifted(cotangent, "pipe", -1)
    return (
        produced[None],
        cotangent[None],
        passed_forward[None],
        passed_backward[None],
        gain_total[None],
    )


def solution(mesh):
    placed = (
        P("pipe", "dp", "expert"),
        P("pipe", "dp", "expert"),
        P("pipe", "dp", "expert"),
        P("pipe", "dp", None),
        P("pipe", "dp", None),
        P("pipe", "expert"),
        P("pipe", "expert", None),
        P("pipe", "dp", None, None, "expert"),
        P("pipe", "dp", "expert", None),
    )
    return jax.shard_map(
        local,
        mesh=mesh,
        in_specs=placed,
        out_specs=(
            P("pipe", "dp", "expert"),
            P("pipe", "dp", "expert"),
            P("pipe", "dp", "expert"),
            P("pipe", "dp", "expert"),
            P("pipe", "expert"),
        ),
        check_vma=False,
    )
```
